32 devices in a mesh: gx: 4 (over z), gy: 2 (over y), gz: 4 (over x, core).
Axes of the slice: x: 2, y: 2, z: 4, core: 2. Of those that a mesh axis runs over, the one named last changes fastest.
Arguments:
- density: float32 [32, 16, 512], P('gx', 'gy', 'gz'), may hold values from 0.5 to 2
- base_velocity: float32 [3, 32, 16, 512], P(None, 'gx', 'gy', 'gz'), may hold values from -0.4 to 0.4
- cells: int32 [3, 8192], P(None, ('gx', 'gy', 'gz')), may hold values from 0 to 511, as said below
- offsets: float32 [3, 8192], P(None, ('gx', 'gy', 'gz')), may hold values from 0 to 1
- target: float32 [3, 8192], P(None, ('gx', 'gy', 'gz')), may hold values from -0.4 to 0.4
- stiffness: float32 [8192], P(('gx', 'gy', 'gz')), may hold values from 0.01 to 0.1
- counts: int32 [32], P(('gx', 'gy', 'gz')), may hold values from 1 to 256, as said below
Outputs:
- forces: float32 [3, 8192], P(None, ('gx', 'gy', 'gz'))
The draws below stay inside these ranges and needn't reach their ends.
Inputs may be any that keep to these rules, and one draw needn't show every extreme that they name: `cells`: each marker's cell lies inside the lattice block of the device that holds its slot. `counts`: some device holds exactly 256 live markers in every draw.
All inputs are finite; a program needn't handle non-finite values.
Results may differ from the reference program's by a relative error of at most 0.0001.
Values sent between devices are 32-bit elements; how exact they have to be, the bound alone decides.
A program may use at most 64 MiB of HBM per device.

```python
import math
import jax
import jax.numpy as jnp
from jax import lax

CX = 8
CY = 8
CZ = 128
CAP = 256
ITERS = 3
NX = 32
NY = 16
NZ = 512
SLOTS = 8192
DEVICES = 32


def draw_cells(key, part):
    blocks_y = NY // CY
    blocks_z = NZ // CZ
    device = jnp.arange(SLOTS, dtype=jnp.int32) // CAP
    block_x = device // (blocks_y * blocks_z)
    block_y = device // blocks_z % blocks_y
    block_z = device % blocks_z
    keys = jax.random.split(key, 3)
    inside_x = jax.random.randint(keys[0], (SLOTS,), 0, CX, dtype=jnp.int32)
    inside_y = jax.random.randint(keys[1], (SLOTS,), 0, CY, dtype=jnp.int32)
    inside_z = jax.random.randint(keys[2], (SLOTS,), 0, CZ, dtype=jnp.int32)
    return jnp.stack([block_x * CX + inside_x, block_y * CY + inside_y, block_z * CZ + inside_z]).astype(jnp.int32)


def draw_counts(key, part):
    keys = jax.random.split(key, 3)
    divisor = 1 + jax.random.randint(keys[0], (DEVICES,), 0, 6, dtype=jnp.int32)
    jitter = jax.random.randint(keys[1], (DEVICES,), 0, CAP // 8 + 1, dtype=jnp.int32)
    loads = jnp.maximum(CAP // divisor - jitter, 1)
    fullest = jax.random.randint(keys[2], (), 0, DEVICES, dtype=jnp.int32)
    loads = jnp.where(jnp.arange(DEVICES, dtype=jnp.int32) == fullest, CAP, loads)
    return loads.astype(jnp.int32)


def levels(stream_key, extent, shards, low, largest):
    level, own = 1.0, jax.random.fold_in(stream_key, 6)
    for axis_at, blocks in shards:
        steps = jnp.exp(jax.random.uniform(jax.random.fold_in(own, axis_at), (blocks,), jnp.float32, low / len(shards), largest / len(shards)))
        level = level * jnp.repeat(steps, extent[axis_at] // blocks).reshape([-1 if axis == axis_at else 1 for axis in range(len(extent))])
    return level


def normal_values(stream_key, dims, scale, limit, shards=(), kind=jnp.bfloat16):
    values = scale * jax.random.normal(stream_key, dims, jnp.float32)
    if shards:
        values = values * levels(stream_key, dims, shards, -0.22, 0.18)
    return jnp.clip(values, -limit, limit).astype(kind)


def setup_inputs(seed: int = 0) -> dict:
    seeds = jax.random.split(jax.random.key(seed), 8)
    return {
        "density": jnp.clip(jnp.exp(math.log(2.0) - 1.3862944 * jax.random.uniform(seeds[0], (NX, NY, NZ), jnp.float32) ** levels(seeds[0], (NX, NY, NZ), ((0, 4), (1, 2), (2, 4)), -0.2, 0.2)), 0.5, 2.0),
        "base_velocity": normal_values(seeds[1], (3, NX, NY, NZ), 0.05, 0.4, ((1, 4), (2, 2), (3, 4)), jnp.float32),
        "cells": draw_cells(jax.random.fold_in(seeds[7], 71), 0),
        "offsets": jnp.clip(1.0 * jax.random.uniform(seeds[3], (3, SLOTS), jnp.float32) ** levels(seeds[3], (3, SLOTS), ((1, 32),), -0.2, 0.2), 0.0, 1.0),
        "target": normal_values(seeds[4], (3, SLOTS), 0.05, 0.4, ((1, 32),), jnp.float32),
        "stiffness": jnp.clip(jnp.exp(math.log(0.1) - 2.3025851 * jax.random.uniform(seeds[5], (SLOTS,), jnp.float32) ** levels(seeds[5], (SLOTS,), ((0, 32),), -0.2, 0.2)), 0.01, 0.1),
        "counts": draw_counts(jax.random.fold_in(seeds[7], 71), 0),
    }


def moving_directions():
    listing = []
    for along_x in (-1, 0, 1):
        for along_y in (-1, 0, 1):
            for along_z in (-1, 0, 1):
                order = abs(along_x) + abs(along_y) + abs(along_z)
                if order == 1:
                    listing.append((along_x, along_y, along_z, 1.0 / 18.0))
                elif order == 2:
                    listing.append((along_x, along_y, along_z, 1.0 / 36.0))
    return listing

def delta_weights(fraction):

    def inner(radius):
        return (3.0 - 2.0 * radius + jnp.sqrt(1.0 + 4.0 * radius - 4.0 * radius * radius)) / 8.0

    def outer(radius):
        return (5.0 - 2.0 * radius - jnp.sqrt(-7.0 + 12.0 * radius - 4.0 * radius * radius)) / 8.0
    return jnp.stack([outer(1.0 + fraction), inner(fraction), inner(1.0 - fraction), outer(2.0 - fraction)])

def reference(density, base_velocity, cells, offsets, target, stiffness, counts):
    live = (jnp.arange(CAP, dtype=jnp.int32)[None, :] < counts[:, None]).reshape(-1).astype(jnp.float32)
    scale = lax.rsqrt(density)
    weight_x = delta_weights(offsets[0])
    weight_y = delta_weights(offsets[1])
    weight_z = delta_weights(offsets[2])
    index_x = [((cells[0] + shift - 1) % NX).astype(jnp.int32) for shift in range(4)]
    index_y = [((cells[1] + shift - 1) % NY).astype(jnp.int32) for shift in range(4)]
    index_z = [((cells[2] + shift - 1) % NZ).astype(jnp.int32) for shift in range(4)]
    directions = moving_directions()

    def interpolate(field):
        total = jnp.zeros((3, SLOTS), jnp.float32)
        for first in range(4):
            for second in range(4):
                for third in range(4):
                    weight = weight_x[first] * weight_y[second] * weight_z[third]
                    total = total + field[:, index_x[first], index_y[second], index_z[third]] * weight
        return total

    def spread(vector):
        grid = jnp.zeros((3, NX, NY, NZ), jnp.float32)
        for first in range(4):
            for second in range(4):
                for third in range(4):
                    weight = weight_x[first] * weight_y[second] * weight_z[third]
                    grid = grid.at[:, index_x[first], index_y[second], index_z[third]].add(vector * weight)
        return grid

    def apply(vector):
        moved = scale * spread(vector)
        post = [jnp.zeros((NX, NY, NZ), jnp.float32) for component in range(3)]
        for along_x, along_y, along_z, share in directions:
            population = 3.0 * share * (along_x * moved[0] + along_y * moved[1] + along_z * moved[2])
            shifted = jnp.roll(population, (along_x, along_y, along_z), axis=(0, 1, 2))
            for component, along in enumerate((along_x, along_y, along_z)):
                if along != 0:
                    post[component] = post[component] + along * shifted
        velocity = scale * (moved + jnp.stack(post)) * 0.5
        return live * (interpolate(velocity) + stiffness * vector)
    right = live * (target - interpolate(base_velocity))
    solution = jnp.zeros_like(right)
    residual = right
    direction = right
    norm_now = jnp.sum(residual * residual)
    for step in range(ITERS):
        image = apply(direction)
        alpha = norm_now / jnp.sum(direction * image)
        solution = solution + alpha * direction
        residual = residual - alpha * image
        norm_next = jnp.sum(residual * residual)
        direction = residual + norm_next / norm_now * direction
        norm_now = norm_next
    return solution
```

```python
import functools
import itertools

import jax
import jax.numpy as jnp
from jax import lax
from jax.experimental import pallas as pl
from jax.experimental.pallas import tpu as pltpu
from jax.sharding import PartitionSpec as P

ITERS = 3
MOST_DIRECT = 64
LOW, HIGH = 2, 3
MESH_ID = pl.DeviceIdType.MESH
AXES = ("gx", "gy", "gz")


def round_up(value, multiple):
    return -(-value // multiple) * multiple


def axis_groups(count):
    groups = {}
    for shift in (0, -1, 1):
        groups.setdefault(shift % count, []).append(shift)
    return list(groups.items())


def span(shifts, size):
    if shifts == [0]:
        return 1, size + 3
    if shifts == [-1]:
        return 0, 4
    if shifts == [1]:
        return size + 1, 4
    return 0, size + 5


def weights(fraction):
    root = jnp.sqrt(1.0 + 4.0 * fraction - 4.0 * fraction * fraction)
    near, far = 3.0 - 2.0 * fraction, 1.0 + 2.0 * fraction
    return ((near - root) / 8.0, (near + root) / 8.0, (far + root) / 8.0, (far - root) / 8.0)


def table(cell, four, shifts, size, first, rows):
    place = lax.broadcasted_iota(jnp.int32, (rows, cell.shape[1]), 0).astype(jnp.float32) + first
    total = None
    for shift in shifts:
        apart = place - (cell + (1.0 + shift * size))
        part = jnp.where(apart == 3.0, four[3], 0.0)
        for number in (2, 1, 0):
            part = jnp.where(apart == float(number), four[number], part)
        total = part if total is None else total + part
    return total


def split(value):
    high = value.astype(jnp.bfloat16)
    return high, (value - high.astype(jnp.float32)).astype(jnp.bfloat16)


def dot_nt(a, b):
    return lax.dot_general(a, b, (((1,), (1,)), ((), ())), preferred_element_type=jnp.float32)


def dot_nn(a, b):
    return lax.dot_general(a, b, (((1,), (0,)), ((), ())), preferred_element_type=jnp.float32)


def kernel(
    counts, sizes, density_in, velocity_in, cells_in, offsets_in, target_in, stiffness_in, live_in, out,
    block, dense, cell, offset, target, stiffness, held, fields, xbuf, ybuf, zpack, zbuf, nbuf, fbuf, rbuf, dbuf, txy, thi, tlo, whi, wlo,
    grid, lsem, nsend, nrecv, rsend, rrecv, dsend, drecv, hsend, hrecv,
):
    size_x, size_y, size_z = sizes
    cap = cell.shape[1]
    rows_y, lanes = fields.shape[2], fields.shape[3]
    assert 8 * (size_x + 5) <= size_z == lanes - size_z
    wide_x = size_x + 5
    groups = [axis_groups(count) for count in counts]
    slots = list(itertools.product(*[[offset for offset, _ in group] for group in groups]))
    me = [lax.axis_index(name) for name in AXES]
    sent = []

    def device(offset):
        return tuple(lax.rem(m + o, n) for m, o, n in zip(me, offset, counts))

    def negated(offset):
        return tuple((-o) % n for o, n in zip(offset, counts))

    peers = {slot for slot in slots if any(slot)}
    for axis, count in enumerate(counts):
        for step in range(1, count):
            peers.add(tuple(step if a == axis else 0 for a in range(3)))
    everyone = [o for o in itertools.product(*[range(n) for n in counts]) if any(o)]
    direct = len(everyone) < MOST_DIRECT
    peers = everyone if direct else sorted(peers)
    loads = [
        pltpu.make_async_copy(source, target_ref, lsem.at[number])
        for number, (source, target_ref) in enumerate((
            (density_in, dense), (velocity_in, block.at[pl.ds(0, 3)]), (cells_in, cell), (offsets_in, offset),
            (target_in, target), (stiffness_in, stiffness), (live_in, held),
        ))
    ]
    barrier = pltpu.get_barrier_semaphore()
    for peer in peers:
        pl.semaphore_signal(barrier, inc=1, device_id=device(peer), device_id_type=MESH_ID)
    for load in loads:
        load.start()
    for load in loads:
        load.wait()
    block[3] = lax.rsqrt(dense[...])
    corner = [m * size for m, size in zip(me, sizes)]
    for k in range(3):
        nbuf[0, pl.ds(k, 1), :] = (cell[pl.ds(k, 1), :] - corner[k]).astype(jnp.float32)
    nbuf[0, pl.ds(3, 3), :] = offset[...]
    nbuf[0, pl.ds(6, 2), :] = jnp.zeros((2, cap), jnp.float32)
    live = (lax.broadcasted_iota(jnp.int32, (1, cap), 1) < held[0]).astype(jnp.float32)
    pl.semaphore_wait(barrier, len(peers))

    def neighbour_copy(turn, number):
        return pltpu.make_async_remote_copy(
            src_ref=fbuf.at[turn - 1, 0] if turn else nbuf.at[0],
            dst_ref=fbuf.at[turn - 1, number] if turn else nbuf.at[number],
            send_sem=nsend.at[turn, number - 1],
            recv_sem=nrecv.at[turn, number - 1],
            device_id=device(negated(slots[number])),
            device_id_type=MESH_ID,
        )

    def send_round(turn):
        for number in sorted(range(1, len(slots)), key=lambda k: (slots[k][0] == 0, k)):
            copy = neighbour_copy(turn, number)
            copy.start()
            sent.append(copy)

    def wait_round(turn, off_x):
        for number in range(1, len(slots)):
            if slots[number][0] == off_x:
                neighbour_copy(turn, number).wait_recv()

    def sum_copy(turn, stage, step):
        axis = 2 - stage
        offset = tuple((-step) % counts[axis] if a == axis else 0 for a in range(3))
        return pltpu.make_async_remote_copy(
            src_ref=rbuf.at[turn, stage, 0],
            dst_ref=rbuf.at[turn, stage, step],
            send_sem=rsend.at[turn, stage, step - 1],
            recv_sem=rrecv.at[turn, stage, step - 1],
            device_id=device(offset),
            device_id_type=MESH_ID,
        )

    def send_sum(turn, stage, value):
        rbuf[turn, stage, 0] = value
        for step in range(1, counts[2 - stage]):
            copy = sum_copy(turn, stage, step)
            copy.start()
            sent.append(copy)

    def wait_sum(turn, stage):
        for step in range(1, counts[2 - stage]):
            sum_copy(turn, stage, step).wait_recv()
        total = rbuf[turn, stage, 0]
        for step in range(1, counts[2 - stage]):
            total = total + rbuf[turn, stage, step]
        return total

    def put(turn, vector):
        for c in range(3):
            for part in range(cap // 128):
                fbuf[turn - 1, 0, pl.ds(c * (cap // 128) + part, 1), :] = vector[
                    c : c + 1, part * 128 : part * 128 + 128
                ]

    def taken(turn, number, c):
        each = cap // 128
        return jnp.concatenate(
            [fbuf[turn - 1, number, pl.ds(c * each + part, 1), :] for part in range(each)], axis=1
        )

    def direct_copy(step, number):
        return pltpu.make_async_remote_copy(
            src_ref=dbuf.at[step, 0],
            dst_ref=dbuf.at[step, number + 1],
            send_sem=dsend.at[step, number],
            recv_sem=drecv.at[step, number],
            device_id=device(negated(everyone[number])),
            device_id_type=MESH_ID,
        )

    def send_directly(step, value):
        dbuf[step, 0] = value
        for number in range(len(everyone)):
            copy = direct_copy(step, number)
            copy.start()
            sent.append(copy)

    def wait_directly(step):
        for number in range(len(everyone)):
            direct_copy(step, number).wait_recv()
        return jnp.sum(dbuf[step], axis=0)

    offs_y = sorted({1 % counts[1], (-1) % counts[1]})
    offs_z = sorted({1 % counts[2], (-1) % counts[2]})

    def halo_copy(number, source, target, offset):
        return pltpu.make_async_remote_copy(
            src_ref=source,
            dst_ref=target,
            send_sem=hsend.at[number],
            recv_sem=hrecv.at[number],
            device_id=device(negated(offset)),
            device_id_type=MESH_ID,
        )

    def go(copies):
        for copy in copies:
            copy.start()
            sent.append(copy)

    low, high = pl.ds(0, LOW), pl.ds(LOW, HIGH)
    along_x = [
        halo_copy(0, block.at[:, pl.ds(size_x - LOW, LOW)], xbuf.at[:, low], (counts[0] - 1, 0, 0)),
        halo_copy(1, block.at[:, pl.ds(0, HIGH)], xbuf.at[:, high], (1, 0, 0)),
    ]
    along_y, relayed_y = [], []
    for k, off in enumerate(offs_y):
        here = (0, off, 0)
        along_y.append(halo_copy(2 + k, block, ybuf.at[k, :, pl.ds(LOW, size_x)], here))
        relayed_y.append(halo_copy(4 + k, xbuf.at[:, low], ybuf.at[k, :, low], here))
        relayed_y.append(
            halo_copy(6 + k, xbuf.at[:, high], ybuf.at[k, :, pl.ds(LOW + size_x, HIGH)], here)
        )
    along_z = [halo_copy(8 + k, zpack, zbuf.at[k], (0, 0, off)) for k, off in enumerate(offs_z)]

    def widen():
        for copy in along_y + relayed_y:
            copy.wait_recv()
        below = ybuf.at[offs_y.index((-1) % counts[1])]
        above = ybuf.at[offs_y.index(1 % counts[1])]
        lane = lax.broadcasted_iota(jnp.int32, (4, rows_y, size_z), 2)
        zero = jnp.zeros((4, rows_y - size_y - LOW - HIGH, size_z), jnp.float32)
        packed = jnp.zeros((4, rows_y, size_z), jnp.float32)
        for plane in range(wide_x):
            if plane < LOW:
                own = xbuf[:, plane]
            elif plane < LOW + size_x:
                own = block[:, plane - LOW]
            else:
                own = xbuf[:, plane - size_x]
            tall = jnp.concatenate(
                [below[:, plane][:, size_y - LOW :], own, above[:, plane][:, :HIGH], zero], axis=1
            )
            fields[:, plane, :, pl.ds(0, size_z)] = tall
            ends = jnp.where(lane < HIGH, tall, pltpu.roll(tall, LOW + HIGH, 2))
            at = 8 * plane
            inside = (lane >= at) & (lane < at + LOW + HIGH)
            packed = jnp.where(inside, pltpu.roll(ends, at, 2) if at else ends, packed)
        zpack[...] = packed
        go(along_z)
        for copy in along_z:
            copy.wait_recv()
        before = zbuf[offs_z.index((-1) % counts[2])]
        after = zbuf[offs_z.index(1 % counts[2])]
        for plane in range(wide_x):
            at = 8 * plane
            tall = pltpu.roll(fields[:, plane, :, pl.ds(0, size_z)], LOW, 2)
            first = pltpu.roll(before, (-(at + HIGH)) % size_z, 2)
            last = pltpu.roll(after, (LOW - at) % size_z, 2)
            fields[:, plane, :, pl.ds(0, size_z)] = jnp.where(lane < LOW, first, tall)
            tail = jnp.where(lane < LOW, tall, jnp.where(lane < LOW + HIGH, last, 0.0))
            fields[:, plane, :, pl.ds(size_z, lanes - size_z)] = tail

    go(along_x + along_y)
    send_round(0)

    def build(xi, yi, zi):
        number = slots.index((groups[0][xi][0], groups[1][yi][0], groups[2][zi][0]))
        info = nbuf[number]
        cells = [info[k : k + 1] for k in range(3)]
        fours = [weights(info[k + 3 : k + 4]) for k in range(3)]
        block = (yi * len(groups[2]) + zi) * cap
        start, planes = span(groups[0][xi][1], size_x)
        first = start // 8 * 8
        tall = round_up(start + planes - first, 8)
        tab_x = table(cells[0], fours[0], groups[0][xi][1], size_x, float(first), tall)
        tab_y = table(cells[1], fours[1], groups[1][yi][1], size_y, 0.0, rows_y)
        for plane in range(planes):
            at = start - first + plane
            txy[xi, pl.ds(plane * rows_y, rows_y), pl.ds(block, cap)] = tab_x[at : at + 1] * tab_y
        shifts = groups[2][zi][1]
        start, planes = span(shifts, size_z)
        first = start // 16 * 16
        tall = round_up(start + planes - first, 16)
        tab_z = table(cells[2], fours[2], shifts, size_z, float(first), tall)
        high, low = split(tab_z)
        for ref, part in ((thi, high), (tlo, low)):
            if first:
                ref[xi, pl.ds(0, first), pl.ds(block, cap)] = jnp.zeros((first, cap), jnp.bfloat16)
            ref[xi, pl.ds(first, tall), pl.ds(block, cap)] = part
            rest = lanes - first - tall
            if rest:
                ref[xi, pl.ds(first + tall, rest), pl.ds(block, cap)] = jnp.zeros(
                    (rest, cap), jnp.bfloat16
                )

    start_own, planes_own = span(groups[0][0][1], size_x)

    def interpolate(field):
        rows = planes_own * rows_y
        high, low = split(field.reshape(3 * rows, lanes))
        z_high, z_low = thi[0, :, pl.ds(0, cap)], tlo[0, :, pl.ds(0, cap)]
        part = dot_nn(high, z_high) + dot_nn(low, z_high) + dot_nn(high, z_low)
        plane = txy[0, pl.ds(0, rows), pl.ds(0, cap)]
        return jnp.concatenate(
            [
                jnp.sum(part[c * rows : (c + 1) * rows] * plane, axis=0, keepdims=True)
                for c in range(3)
            ],
            axis=0,
        )

    def spread(turn):
        for xi, (off_x, shifts) in enumerate(groups[0]):
            start, planes = span(shifts, size_x)
            rows = planes * rows_y
            wait_round(turn, off_x)
            for yi, (off_y, _) in enumerate(groups[1]):
                for zi, (off_z, _) in enumerate(groups[2]):
                    number = slots.index((off_x, off_y, off_z))
                    block = (yi * len(groups[2]) + zi) * cap
                    plane = txy[xi, pl.ds(0, rows), pl.ds(block, cap)]
                    for c in range(3):
                        high, low = split(plane * taken(turn, number, c))
                        whi[pl.ds(c * rows, rows), pl.ds(block, cap)] = high
                        wlo[pl.ds(c * rows, rows), pl.ds(block, cap)] = low
            high, low = whi[pl.ds(0, 3 * rows), :], wlo[pl.ds(0, 3 * rows), :]
            part = dot_nt(high, thi[xi]) + dot_nt(low, thi[xi]) + dot_nt(high, tlo[xi])
            part = part.reshape(3, planes, rows_y, lanes)
            if xi == 0:
                if start > 0:
                    grid[:, pl.ds(0, start)] = jnp.zeros((3, start, rows_y, lanes), jnp.float32)
                rest = wide_x - start - planes
                if rest > 0:
                    grid[:, pl.ds(start + planes, rest)] = jnp.zeros(
                        (3, rest, rows_y, lanes), jnp.float32
                    )
                grid[:, pl.ds(start, planes)] = part
            else:
                grid[:, pl.ds(start, planes)] += part

    def shifted(value, by, axis):
        return pltpu.roll(value, by % value.shape[axis], axis)

    def both(value, axis):
        return shifted(value, -1, axis), shifted(value, 1, axis)

    def add(value, axis):
        up, down = both(value, axis)
        return up + down

    def sub(value, axis):
        up, down = both(value, axis)
        return up - down

    def respond():
        scale = fields[3]
        mx, my, mz = (scale * grid[c] for c in range(3))
        slope_y, slope_z = sub(my, 1), sub(mz, 2)
        sum_x = 2.0 * mx + add(mx, 1) + add(mx, 2)
        slope = slope_y + slope_z
        px = sum_x[2:] + sum_x[:-2] + slope[2:] - slope[:-2]
        slope_x = mx[2:] - mx[:-2]
        sum_y = (2.0 * my + add(my, 2))[1:-1] + my[2:] + my[:-2]
        py = add(sum_y, 1) + sub(slope_x + slope_z[1:-1], 1)
        sum_z = (2.0 * mz + add(mz, 1))[1:-1] + mz[2:] + mz[:-2]
        pz = add(sum_z, 2) + sub(slope_x + slope_y[1:-1], 2)
        half = scale[1:-1] * 0.5
        return jnp.stack(
            [half * (m[1:-1] + p * (1.0 / 12.0)) for m, p in ((mx, px), (my, py), (mz, pz))]
        )

    def apply(turn, vector, summing=None):
        spread(turn)
        if summing is not None:
            send_sum(summing, 1, wait_sum(summing, 0))
        field = respond()
        if summing is not None:
            send_sum(summing, 2, wait_sum(summing, 1))
        return live * (interpolate(field) + stiffness[...] * vector)

    def partial_sums(residual, image):
        folded = []
        for other in (residual, image):
            row = jnp.sum(residual * other, axis=0, keepdims=True)
            total = row[:, :128]
            for at in range(128, cap, 128):
                total = total + row[:, at : at + 128]
            folded.append(total)
        return jnp.concatenate(folded, axis=0)

    def totals(tile):
        return (
            jnp.sum(tile[0:1], axis=1, keepdims=True),
            jnp.sum(tile[1:2], axis=1, keepdims=True),
        )

    build(0, 0, 0)
    for copy in along_x:
        copy.wait_recv()
    go(relayed_y)
    for off_x, _ in groups[0]:
        wait_round(0, off_x)
    for xi, yi, zi in itertools.product(*[range(len(group)) for group in groups]):
        if (xi, yi, zi) != (0, 0, 0):
            build(xi, yi, zi)
    widen()
    residual = live * (target[...] - interpolate(fields[pl.ds(0, 3), pl.ds(1, size_x + 3)]))
    put(1, residual)
    send_round(1)

    image = apply(1, residual)
    direction, along, along_image = residual, image, None
    answer = None
    norm_before = alpha = None
    for step in range(ITERS):
        sums = partial_sums(residual, image)
        if step + 1 < ITERS:
            put(step + 2, image)
            send_round(step + 2)
        if direct:
            send_directly(step, sums)
            if step + 1 < ITERS:
                ahead = apply(step + 2, image)
            norm, product = totals(wait_directly(step))
        elif step + 1 < ITERS:
            send_sum(step, 0, sums)
            ahead = apply(step + 2, image, step)
            norm, product = totals(wait_sum(step, 2))
        else:
            send_sum(step, 0, sums)
            send_sum(step, 1, wait_sum(step, 0))
            send_sum(step, 2, wait_sum(step, 1))
            norm, product = totals(wait_sum(step, 2))
        if step == 0:
            alpha = norm / product
            along_image = ahead
        else:
            ratio = norm / norm_before
            alpha = norm / (product - ratio * norm / alpha)
            direction = residual + ratio * direction
            if step + 1 < ITERS:
                along = image + ratio * along
                along_image = ahead + ratio * along_image
        answer = alpha * direction if answer is None else answer + alpha * direction
        norm_before = norm
        if step + 1 < ITERS:
            residual = residual - alpha * along
            image = image - alpha * along_image
    out[...] = answer
    for copy in sent:
        copy.wait_send()


def body(mesh_counts, density, base_velocity, cells, offsets, target, stiffness, counts):
    sizes = density.shape
    size_x, size_y, size_z = sizes
    cap = cells.shape[1]
    rows_y, lanes = round_up(size_y + 5, 16), round_up(size_z + 5, 128)
    groups = [axis_groups(count) for count in mesh_counts]
    number = len(groups[0]) * len(groups[1]) * len(groups[2])
    width = len(groups[1]) * len(groups[2]) * cap
    tallest = max(span(shifts, size_x)[1] for _, shifts in groups[0])
    longest = max(mesh_counts)
    turns = ITERS + 1
    devices = mesh_counts[0] * mesh_counts[1] * mesh_counts[2]
    most = devices if devices <= MOST_DIRECT else 1
    return pl.pallas_call(
        functools.partial(kernel, mesh_counts, sizes),
        out_shape=jax.ShapeDtypeStruct((3, cap), jnp.float32),
        in_specs=[pl.BlockSpec(memory_space=pltpu.HBM)] * 7,
        out_specs=pl.BlockSpec(memory_space=pltpu.VMEM),
        scratch_shapes=[
            pltpu.VMEM((4, size_x, size_y, size_z), jnp.float32),
            pltpu.VMEM((size_x, size_y, size_z), jnp.float32),
            pltpu.VMEM((3, cap), jnp.int32),
            pltpu.VMEM((3, cap), jnp.float32),
            pltpu.VMEM((3, cap), jnp.float32),
            pltpu.VMEM((1, cap), jnp.float32),
            pltpu.SMEM((1,), jnp.int32),
            pltpu.VMEM((4, size_x + 5, rows_y, lanes), jnp.float32),
            pltpu.VMEM((4, LOW + HIGH, size_y, size_z), jnp.float32),
            pltpu.VMEM((2, 4, size_x + 5, size_y, size_z), jnp.float32),
            pltpu.VMEM((4, rows_y, size_z), jnp.float32),
            pltpu.VMEM((2, 4, rows_y, size_z), jnp.float32),
            pltpu.VMEM((number, 8, cap), jnp.float32),
            pltpu.VMEM((ITERS, number, 3 * (cap // 128), 128), jnp.float32),
            pltpu.VMEM((ITERS, 3, longest, 2, 128), jnp.float32),
            pltpu.VMEM((ITERS, most, 2, 128), jnp.float32),
            pltpu.VMEM((len(groups[0]), tallest * rows_y, width), jnp.float32),
            pltpu.VMEM((len(groups[0]), lanes, width), jnp.bfloat16),
            pltpu.VMEM((len(groups[0]), lanes, width), jnp.bfloat16),
            pltpu.VMEM((3 * tallest * rows_y, width), jnp.bfloat16),
            pltpu.VMEM((3 * tallest * rows_y, width), jnp.bfloat16),
            pltpu.VMEM((3, size_x + 5, rows_y, lanes), jnp.float32),
            pltpu.SemaphoreType.DMA((7,)),
            pltpu.SemaphoreType.DMA((turns, number - 1)),
            pltpu.SemaphoreType.DMA((turns, number - 1)),
            pltpu.SemaphoreType.DMA((ITERS, 3, longest - 1)),
            pltpu.SemaphoreType.DMA((ITERS, 3, longest - 1)),
            pltpu.SemaphoreType.DMA((ITERS, most)),
            pltpu.SemaphoreType.DMA((ITERS, most)),
            pltpu.SemaphoreType.DMA((10,)),
            pltpu.SemaphoreType.DMA((10,)),
        ],
        compiler_params=pltpu.CompilerParams(
            collective_id=0, has_side_effects=True, vmem_limit_bytes=60 * 1024 * 1024
        ),
    )(density, base_velocity, cells, offsets, target, stiffness[None], counts)


def solution(mesh):
    return jax.shard_map(
        functools.partial(body, tuple(mesh.shape[name] for name in AXES)),
        mesh=mesh,
        in_specs=(
            P("gx", "gy", "gz"),
            P(None, "gx", "gy", "gz"),
            P(None, ("gx", "gy", "gz")),
            P(None, ("gx", "gy", "gz")),
            P(None, ("gx", "gy", "gz")),
            P(("gx", "gy", "gz")),
            P(("gx", "gy", "gz")),
        ),
        out_specs=P(None, ("gx", "gy", "gz")),
        check_vma=False,
    )
```

```python
import functools
import itertools

import jax
import jax.numpy as jnp
from jax import lax
from jax.experimental import pallas as pl
from jax.experimental.pallas import tpu as pltpu
from jax.sharding import PartitionSpec as P

ITERS = 3
MOST_DIRECT = 64
LOW, HIGH = 2, 3
MESH_ID = pl.DeviceIdType.MESH
AXES = ("gx", "gy", "gz")


def round_up(value, multiple):
    return -(-value // multiple) * multiple


def axis_groups(count):
    groups = {}
    for shift in (0, -1, 1):
        groups.setdefault(shift % count, []).append(shift)
    return list(groups.items())


def span(shifts, size):
    if shifts == [0]:
        return 1, size + 3
    if shifts == [-1]:
        return 0, 4
    if shifts == [1]:
        return size + 1, 4
    return 0, size + 5


def weights(fraction):
    root = jnp.sqrt(1.0 + 4.0 * fraction - 4.0 * fraction * fraction)
    near, far = 3.0 - 2.0 * fraction, 1.0 + 2.0 * fraction
    return ((near - root) / 8.0, (near + root) / 8.0, (far + root) / 8.0, (far - root) / 8.0)


def table(cell, four, shifts, size, first, rows):
    place = lax.broadcasted_iota(jnp.int32, (rows, cell.shape[1]), 0).astype(jnp.float32) + first
    total = None
    for shift in shifts:
        apart = place - (cell + (1.0 + shift * size))
        part = jnp.where(apart == 3.0, four[3], 0.0)
        for number in (2, 1, 0):
            part = jnp.where(apart == float(number), four[number], part)
        total = part if total is None else total + part
    return total


def split(value):
    high = value.astype(jnp.bfloat16)
    return high, (value - high.astype(jnp.float32)).astype(jnp.bfloat16)


def dot_nt(a, b):
    return lax.dot_general(a, b, (((1,), (1,)), ((), ())), preferred_element_type=jnp.float32)


def dot_nn(a, b):
    return lax.dot_general(a, b, (((1,), (0,)), ((), ())), preferred_element_type=jnp.float32)


def kernel(
    counts, sizes, density_in, velocity_in, cells_in, offsets_in, target_in, stiffness_in, live_in, out,
    block, dense, cell, offset, target, stiffness, held, fields, xbuf, ybuf, zpack, zbuf, nbuf, fbuf, rbuf, dbuf, thi, tlo, tz, tzn, wide,
    planar, grid, lsem, nsend, nrecv, rsend, rrecv, dsend, drecv, hsend, hrecv,
):
    size_x, size_y, size_z = sizes
    cap = cell.shape[1]
    rows_y, lanes = fields.shape[2], fields.shape[3]
    assert 8 * (size_x + 5) <= size_z == lanes - size_z
    wide_x = size_x + 5
    tall_z, wide_xy = planar.shape[1], planar.shape[2]
    groups = [axis_groups(count) for count in counts]
    near_x, near_y, near_z = (len(group) for group in groups)
    flat = near_x * near_y
    places = sorted(
        itertools.product(range(near_x), range(near_y), range(near_z)),
        key=lambda place: (place[2] > 0, place[0], place[2], place[1]),
    )
    slots = [tuple(group[k][0] for group, k in zip(groups, place)) for place in places]
    parts = [(1, flat), (flat, len(slots))]
    me = [lax.axis_index(name) for name in AXES]
    sent = []

    def device(offset):
        return tuple(lax.rem(m + o, n) for m, o, n in zip(me, offset, counts))

    def negated(offset):
        return tuple((-o) % n for o, n in zip(offset, counts))

    peers = {slot for slot in slots if any(slot)}
    for axis, count in enumerate(counts):
        for step in range(1, count):
            peers.add(tuple(step if a == axis else 0 for a in range(3)))
    everyone = [o for o in itertools.product(*[range(n) for n in counts]) if any(o)]
    direct = len(everyone) < MOST_DIRECT
    peers = everyone if direct else sorted(peers)
    loads = [
        pltpu.make_async_copy(source, target_ref, lsem.at[number])
        for number, (source, target_ref) in enumerate((
            (density_in, dense), (velocity_in, block.at[pl.ds(0, 3)]), (cells_in, cell), (offsets_in, offset),
            (target_in, target), (stiffness_in, stiffness), (live_in, held),
        ))
    ]
    barrier = pltpu.get_barrier_semaphore()
    for peer in peers:
        pl.semaphore_signal(barrier, inc=1, device_id=device(peer), device_id_type=MESH_ID)
    for load in loads:
        load.start()
    for load in loads:
        load.wait()
    block[3] = lax.rsqrt(dense[...])
    corner = [m * size for m, size in zip(me, sizes)]
    for k in range(3):
        nbuf[0, pl.ds(k, 1), :] = (cell[pl.ds(k, 1), :] - corner[k]).astype(jnp.float32)
    nbuf[0, pl.ds(3, 3), :] = offset[...]
    nbuf[0, pl.ds(6, 2), :] = jnp.zeros((2, cap), jnp.float32)
    live = (lax.broadcasted_iota(jnp.int32, (1, cap), 1) < held[0]).astype(jnp.float32)
    pl.semaphore_wait(barrier, len(peers))

    def neighbour_copy(turn, number):
        return pltpu.make_async_remote_copy(
            src_ref=fbuf.at[turn - 1, 0] if turn else nbuf.at[0],
            dst_ref=fbuf.at[turn - 1, number] if turn else nbuf.at[number],
            send_sem=nsend.at[min(turn, 1)],
            recv_sem=nrecv.at[turn, int(number >= flat)],
            device_id=device(negated(slots[number])),
            device_id_type=MESH_ID,
        )

    def drain(ref, sem):
        pltpu.make_async_copy(ref, ref, sem).wait()

    def send_round(turn):
        for number in sorted(range(1, len(slots)), key=lambda k: (slots[k][0] == 0, k)):
            neighbour_copy(turn, number).start()

    def wait_round(turn, part):
        first, last = parts[part]
        if first < last:
            at = pl.ds(first, last - first)
            drain(fbuf.at[turn - 1, at] if turn else nbuf.at[at], nrecv.at[turn, part])

    def sum_copy(turn, stage, step):
        axis = 2 - stage
        offset = tuple((-step) % counts[axis] if a == axis else 0 for a in range(3))
        return pltpu.make_async_remote_copy(
            src_ref=rbuf.at[turn, stage, 0],
            dst_ref=rbuf.at[turn, stage, step],
            send_sem=rsend.at[turn, stage, step - 1],
            recv_sem=rrecv.at[turn, stage, step - 1],
            device_id=device(offset),
            device_id_type=MESH_ID,
        )

    def send_sum(turn, stage, value):
        rbuf[turn, stage, 0] = value
        for step in range(1, counts[2 - stage]):
            copy = sum_copy(turn, stage, step)
            copy.start()
            sent.append(copy)

    def wait_sum(turn, stage):
        for step in range(1, counts[2 - stage]):
            sum_copy(turn, stage, step).wait_recv()
        total = rbuf[turn, stage, 0]
        for step in range(1, counts[2 - stage]):
            total = total + rbuf[turn, stage, step]
        return total

    def put(turn, vector):
        for c in range(3):
            for part in range(cap // 128):
                fbuf[turn - 1, 0, pl.ds(c * (cap // 128) + part, 1), :] = vector[
                    c : c + 1, part * 128 : part * 128 + 128
                ]

    def taken(turn, number, c):
        each = cap // 128
        return jnp.concatenate(
            [fbuf[turn - 1, number, pl.ds(c * each + part, 1), :] for part in range(each)], axis=1
        )

    def direct_copy(step, number):
        return pltpu.make_async_remote_copy(
            src_ref=dbuf.at[step, 0],
            dst_ref=dbuf.at[step, number + 1],
            send_sem=dsend.at[0],
            recv_sem=drecv.at[step],
            device_id=device(negated(everyone[number])),
            device_id_type=MESH_ID,
        )

    def send_directly(step, value):
        dbuf[step, 0] = value
        for number in range(len(everyone)):
            direct_copy(step, number).start()

    def wait_directly(step):
        drain(dbuf.at[step, pl.ds(1, len(everyone))], drecv.at[step])
        return jnp.sum(dbuf[step], axis=0)

    offs_y = sorted({1 % counts[1], (-1) % counts[1]})
    offs_z = sorted({1 % counts[2], (-1) % counts[2]})

    def halo_copy(number, source, target, offset):
        return pltpu.make_async_remote_copy(
            src_ref=source,
            dst_ref=target,
            send_sem=hsend.at[number],
            recv_sem=hrecv.at[number],
            device_id=device(negated(offset)),
            device_id_type=MESH_ID,
        )

    def go(copies):
        for copy in copies:
            copy.start()
            sent.append(copy)

    low, high = pl.ds(0, LOW), pl.ds(LOW, HIGH)
    along_x = [
        halo_copy(0, block.at[:, pl.ds(size_x - LOW, LOW)], xbuf.at[:, low], (counts[0] - 1, 0, 0)),
        halo_copy(1, block.at[:, pl.ds(0, HIGH)], xbuf.at[:, high], (1, 0, 0)),
    ]
    along_y, relayed_y = [], []
    for k, off in enumerate(offs_y):
        here = (0, off, 0)
        along_y.append(halo_copy(2 + k, block, ybuf.at[k, :, pl.ds(LOW, size_x)], here))
        relayed_y.append(halo_copy(4 + k, xbuf.at[:, low], ybuf.at[k, :, low], here))
        relayed_y.append(
            halo_copy(6 + k, xbuf.at[:, high], ybuf.at[k, :, pl.ds(LOW + size_x, HIGH)], here)
        )
    along_z = [halo_copy(8 + k, zpack, zbuf.at[k], (0, 0, off)) for k, off in enumerate(offs_z)]

    def widen():
        for copy in along_y + relayed_y:
            copy.wait_recv()
        below = ybuf.at[offs_y.index((-1) % counts[1])]
        above = ybuf.at[offs_y.index(1 % counts[1])]
        lane = lax.broadcasted_iota(jnp.int32, (4, rows_y, size_z), 2)
        zero = jnp.zeros((4, rows_y - size_y - LOW - HIGH, size_z), jnp.float32)
        packed = jnp.zeros((4, rows_y, size_z), jnp.float32)
        for plane in range(wide_x):
            if plane < LOW:
                own = xbuf[:, plane]
            elif plane < LOW + size_x:
                own = block[:, plane - LOW]
            else:
                own = xbuf[:, plane - size_x]
            tall = jnp.concatenate(
                [below[:, plane][:, size_y - LOW :], own, above[:, plane][:, :HIGH], zero], axis=1
            )
            fields[:, plane, :, pl.ds(0, size_z)] = tall
            ends = jnp.where(lane < HIGH, tall, pltpu.roll(tall, LOW + HIGH, 2))
            at = 8 * plane
            inside = (lane >= at) & (lane < at + LOW + HIGH)
            packed = jnp.where(inside, pltpu.roll(ends, at, 2) if at else ends, packed)
        zpack[...] = packed
        go(along_z)
        for copy in along_z:
            copy.wait_recv()
        before = zbuf[offs_z.index((-1) % counts[2])]
        after = zbuf[offs_z.index(1 % counts[2])]
        for plane in range(wide_x):
            at = 8 * plane
            tall = pltpu.roll(fields[:, plane, :, pl.ds(0, size_z)], LOW, 2)
            first = pltpu.roll(before, (-(at + HIGH)) % size_z, 2)
            last = pltpu.roll(after, (LOW - at) % size_z, 2)
            fields[:, plane, :, pl.ds(0, size_z)] = jnp.where(lane < LOW, first, tall)
            tail = jnp.where(lane < LOW, tall, jnp.where(lane < LOW + HIGH, last, 0.0))
            fields[:, plane, :, pl.ds(size_z, lanes - size_z)] = tail
        blank = jnp.zeros((wide_xy - wide_x * rows_y, lanes), jnp.float32)
        for number in range(4):
            level = jnp.concatenate([fields[number].reshape(wide_x * rows_y, lanes), blank], axis=0)
            planar[number] = jnp.transpose(level)[:tall_z]

    go(along_x + along_y)
    send_round(0)

    def reach(xi):
        start, planes = span(groups[0][xi][1], size_x)
        first = start * rows_y // 128 * 128
        return first, round_up((start + planes) * rows_y, 128)

    def build(number):
        xi, yi, zi = places[number]
        info = nbuf[number]
        cells = [info[k : k + 1] for k in range(3)]
        fours = [weights(info[k + 3 : k + 4]) for k in range(3)]
        here = number * cap
        start, planes = span(groups[0][xi][1], size_x)
        tab_x = table(cells[0], fours[0], groups[0][xi][1], size_x, 0.0, round_up(wide_x, 8))
        tab_y = table(cells[1], fours[1], groups[1][yi][1], size_y, 0.0, rows_y)
        low_row, high_row = reach(xi)
        for plane in range(low_row // rows_y, high_row // rows_y):
            at = pl.ds(plane * rows_y, rows_y)
            if start <= plane < start + planes:
                high, low = split(tab_x[plane : plane + 1] * tab_y)
            else:
                high = low = jnp.zeros((rows_y, cap), jnp.bfloat16)
            thi[at, pl.ds(here, cap)] = high
            tlo[at, pl.ds(here, cap)] = low
        shifts = groups[2][zi][1]
        if zi == 0:
            tz[:, pl.ds(here, cap)] = table(cells[2], fours[2], shifts, size_z, 0.0, tall_z)
        else:
            edge = None
            for shift in shifts:
                first = 0.0 if shift < 0 else size_z - 3.0
                part = table(cells[2], fours[2], [shift], size_z, first, 8)
                edge = part if edge is None else edge + part
            tzn[:, pl.ds(here - flat * cap, cap)] = edge

    def interpolate(field):
        high, low = split(field.reshape(3 * tall_z, wide_xy))
        xy_high, xy_low = thi[:, pl.ds(0, cap)], tlo[:, pl.ds(0, cap)]
        part = dot_nn(high, xy_high) + dot_nn(low, xy_high) + dot_nn(high, xy_low)
        along = tz[:, pl.ds(0, cap)]
        return jnp.concatenate(
            [
                jnp.sum(part[c * tall_z : (c + 1) * tall_z] * along, axis=0, keepdims=True)
                for c in range(3)
            ],
            axis=0,
        )

    def fill(number, rows):
        at = pl.ds(number * cap, cap)
        along = tz[:, at]
        for c in range(3):
            high, low = split(along * rows[c])
            wide[pl.ds(c * tall_z, tall_z), at] = high
            wide[pl.ds((3 + c) * tall_z, tall_z), at] = low

    def contract(xi, first, last):
        low_row, high_row = reach(xi)
        row, at = pl.ds(low_row, high_row - low_row), pl.ds(first * cap, (last - first) * cap)
        both_parts = dot_nt(wide[:, at], thi[row, at])
        half = 3 * tall_z
        return both_parts[:half] + both_parts[half:] + dot_nt(wide[pl.ds(0, half), at], tlo[row, at])

    def spread(turn, vector):
        fill(0, [vector[c : c + 1] for c in range(3)])
        own = contract(0, 0, 1)
        wait_round(turn, 0)
        for number in range(1, flat):
            fill(number, [taken(turn, number, c) for c in range(3)])
        if near_y > 1:
            own = own + contract(0, 1, near_y)
        for c in range(3):
            grid[c] = own[c * tall_z : (c + 1) * tall_z]
        for xi in range(1, near_x):
            low_row, high_row = reach(xi)
            side = contract(xi, xi * near_y, (xi + 1) * near_y)
            for c in range(3):
                grid[c, :, pl.ds(low_row, high_row - low_row)] += side[c * tall_z : (c + 1) * tall_z]
        if near_z == 1:
            return
        wait_round(turn, 1)
        each = near_y * (near_z - 1)
        top = (size_z + 1) // 8 * 8
        for xi in range(near_x):
            low_row, high_row = reach(xi)
            row = pl.ds(low_row, high_row - low_row)
            begin = flat + xi * each
            rows = [[], [], []]
            for number in range(begin, begin + each):
                edge = tzn[:, pl.ds((number - flat) * cap, cap)]
                for c in range(3):
                    rows[c].append(edge * taken(turn, number, c))
            value = jnp.concatenate([jnp.concatenate(line, axis=1) for line in rows], axis=0)
            rounded = value.astype(jnp.bfloat16).astype(jnp.float32)
            both_parts = jnp.concatenate([rounded, value - rounded], axis=0).astype(jnp.bfloat16)
            at = pl.ds(begin * cap, each * cap)
            part = dot_nt(both_parts, thi[row, at]) + dot_nt(both_parts, tlo[row, at])
            part = part[:24] + part[24:]
            line = lax.broadcasted_iota(jnp.int32, (8, high_row - low_row), 0)
            for c in range(3):
                edge = part[c * 8 : c * 8 + 8]
                grid[c, pl.ds(0, 8), row] += jnp.where(line < 4, edge, 0.0)
                grid[c, pl.ds(top, 8), row] += pltpu.roll(
                    jnp.where(line < 4, 0.0, edge), (size_z + 1 - top - 4) % 8, 0
                )

    def shifted(value, by, axis):
        return pltpu.roll(value, by % value.shape[axis], axis)

    def both(value, axis):
        return shifted(value, -1, axis), shifted(value, 1, axis)

    def add(value, axis):
        up, down = both(value, axis)
        return up + down

    def respond():
        scale = planar[3]
        mx, my, mz = (scale * grid[c] for c in range(3))

        def along(value, step):
            return pltpu.roll(value, (-step) % wide_xy, 1)

        def paired(total, slope, step):
            return along(total + slope, step) + along(total - slope, -step)

        my_up, my_down = along(my, 1), along(my, -1)
        mz_up, mz_down = shifted(mz, -1, 0), shifted(mz, 1, 0)
        mx_up, mx_down = along(mx, rows_y), along(mx, -rows_y)
        slope_x, slope_y, slope_z = mx_up - mx_down, my_up - my_down, mz_up - mz_down
        px = paired(2.0 * mx + along(mx, 1) + along(mx, -1) + add(mx, 0), slope_y + slope_z, rows_y)
        py = paired(2.0 * my + along(my, rows_y) + along(my, -rows_y) + add(my, 0), slope_x + slope_z, 1)
        sum_z = 2.0 * mz + along(mz, 1) + along(mz, -1) + along(mz, rows_y) + along(mz, -rows_y)
        slope = slope_x + slope_y
        pz = shifted(sum_z + slope, -1, 0) + shifted(sum_z - slope, 1, 0)
        half = scale * 0.5
        return jnp.stack([half * (m + p * (1.0 / 12.0)) for m, p in ((mx, px), (my, py), (mz, pz))])

    def apply(turn, vector, summing=None):
        spread(turn, vector)
        if summing is not None:
            send_sum(summing, 1, wait_sum(summing, 0))
        field = respond()
        if summing is not None:
            send_sum(summing, 2, wait_sum(summing, 1))
        return live * (interpolate(field) + stiffness[...] * vector)

    def partial_sums(residual, image):
        folded = []
        for other in (residual, image):
            row = jnp.sum(residual * other, axis=0, keepdims=True)
            total = row[:, :128]
            for at in range(128, cap, 128):
                total = total + row[:, at : at + 128]
            folded.append(total)
        return jnp.concatenate(folded, axis=0)

    def totals(tile):
        return (
            jnp.sum(tile[0:1], axis=1, keepdims=True),
            jnp.sum(tile[1:2], axis=1, keepdims=True),
        )

    build(0)
    for copy in along_x:
        copy.wait_recv()
    go(relayed_y)
    for part in range(2):
        wait_round(0, part)
    for number in range(1, len(slots)):
        build(number)
    widen()
    residual = live * (target[...] - interpolate(planar[pl.ds(0, 3)]))
    put(1, residual)
    send_round(1)

    image = apply(1, residual)
    direction, along, along_image = residual, image, None
    answer = None
    norm_before = alpha = None
    for step in range(ITERS):
        sums = partial_sums(residual, image)
        if step + 1 < ITERS:
            put(step + 2, image)
            send_round(step + 2)
        if direct:
            send_directly(step, sums)
            if step + 1 < ITERS:
                ahead = apply(step + 2, image)
            norm, product = totals(wait_directly(step))
        elif step + 1 < ITERS:
            send_sum(step, 0, sums)
            ahead = apply(step + 2, image, step)
            norm, product = totals(wait_sum(step, 2))
        else:
            send_sum(step, 0, sums)
            send_sum(step, 1, wait_sum(step, 0))
            send_sum(step, 2, wait_sum(step, 1))
            norm, product = totals(wait_sum(step, 2))
        if step == 0:
            alpha = norm / product
            along_image = ahead
        else:
            ratio = norm / norm_before
            alpha = norm / (product - ratio * norm / alpha)
            direction = residual + ratio * direction
            if step + 1 < ITERS:
                along = image + ratio * along
                along_image = ahead + ratio * along_image
        answer = alpha * direction if answer is None else answer + alpha * direction
        norm_before = norm
        if step + 1 < ITERS:
            residual = residual - alpha * along
            image = image - alpha * along_image
    out[...] = answer
    for copy in sent:
        copy.wait_send()
    if len(slots) > 1:
        at = pl.ds(1, len(slots) - 1)
        drain(nbuf.at[at], nsend.at[0])
        drain(fbuf.at[:, at], nsend.at[1])
    if direct and everyone:
        drain(dbuf.at[:, pl.ds(1, len(everyone))], dsend.at[0])


def body(mesh_counts, density, base_velocity, cells, offsets, target, stiffness, counts):
    sizes = density.shape
    size_x, size_y, size_z = sizes
    cap = cells.shape[1]
    rows_y, lanes = round_up(size_y + 5, 16), round_up(size_z + 5, 128)
    groups = [axis_groups(count) for count in mesh_counts]
    number = len(groups[0]) * len(groups[1]) * len(groups[2])
    flat = len(groups[0]) * len(groups[1])
    tall_z, wide_xy = round_up(size_z + 5, 16), round_up((size_x + 5) * rows_y, 128)
    longest = max(mesh_counts)
    turns = ITERS + 1
    devices = mesh_counts[0] * mesh_counts[1] * mesh_counts[2]
    most = devices if devices <= MOST_DIRECT else 1
    return pl.pallas_call(
        functools.partial(kernel, mesh_counts, sizes),
        out_shape=jax.ShapeDtypeStruct((3, cap), jnp.float32),
        in_specs=[pl.BlockSpec(memory_space=pltpu.HBM)] * 7,
        out_specs=pl.BlockSpec(memory_space=pltpu.VMEM),
        scratch_shapes=[
            pltpu.VMEM((4, size_x, size_y, size_z), jnp.float32),
            pltpu.VMEM((size_x, size_y, size_z), jnp.float32),
            pltpu.VMEM((3, cap), jnp.int32),
            pltpu.VMEM((3, cap), jnp.float32),
            pltpu.VMEM((3, cap), jnp.float32),
            pltpu.VMEM((1, cap), jnp.float32),
            pltpu.SMEM((1,), jnp.int32),
            pltpu.VMEM((4, size_x + 5, rows_y, lanes), jnp.float32),
            pltpu.VMEM((4, LOW + HIGH, size_y, size_z), jnp.float32),
            pltpu.VMEM((2, 4, size_x + 5, size_y, size_z), jnp.float32),
            pltpu.VMEM((4, rows_y, size_z), jnp.float32),
            pltpu.VMEM((2, 4, rows_y, size_z), jnp.float32),
            pltpu.VMEM((number, 8, cap), jnp.float32),
            pltpu.VMEM((ITERS, number, 3 * (cap // 128), 128), jnp.float32),
            pltpu.VMEM((ITERS, 3, longest, 2, 128), jnp.float32),
            pltpu.VMEM((ITERS, most, 2, 128), jnp.float32),
            pltpu.VMEM((wide_xy, number * cap), jnp.bfloat16),
            pltpu.VMEM((wide_xy, number * cap), jnp.bfloat16),
            pltpu.VMEM((tall_z, flat * cap), jnp.float32),
            pltpu.VMEM((8, max(1, len(groups[2]) - 1) * flat * cap), jnp.float32),
            pltpu.VMEM((6 * tall_z, flat * cap), jnp.bfloat16),
            pltpu.VMEM((4, tall_z, wide_xy), jnp.float32),
            pltpu.VMEM((3, tall_z, wide_xy), jnp.float32),
            pltpu.SemaphoreType.DMA((7,)),
            pltpu.SemaphoreType.DMA((2,)),
            pltpu.SemaphoreType.DMA((turns, 2)),
            pltpu.SemaphoreType.DMA((ITERS, 3, longest - 1) if most == 1 else (1, 1, 1)),
            pltpu.SemaphoreType.DMA((ITERS, 3, longest - 1) if most == 1 else (1, 1, 1)),
            pltpu.SemaphoreType.DMA((1,)),
            pltpu.SemaphoreType.DMA((ITERS,)),
            pltpu.SemaphoreType.DMA((10,)),
            pltpu.SemaphoreType.DMA((10,)),
        ],
        compiler_params=pltpu.CompilerParams(
            collective_id=0, has_side_effects=True, vmem_limit_bytes=60 * 1024 * 1024
        ),
    )(density, base_velocity, cells, offsets, target, stiffness[None], counts)


def solution(mesh):
    return jax.shard_map(
        functools.partial(body, tuple(mesh.shape[name] for name in AXES)),
        mesh=mesh,
        in_specs=(
            P("gx", "gy", "gz"),
            P(None, "gx", "gy", "gz"),
            P(None, ("gx", "gy", "gz")),
            P(None, ("gx", "gy", "gz")),
            P(None, ("gx", "gy", "gz")),
            P(("gx", "gy", "gz")),
            P(("gx", "gy", "gz")),
        ),
        out_specs=P(None, ("gx", "gy", "gz")),
        check_vma=False,
    )
```

```python
import functools
import itertools

import jax
import jax.numpy as jnp
from jax import lax
from jax.experimental import pallas as pl
from jax.experimental.pallas import tpu as pltpu
from jax.sharding import PartitionSpec as P

ITERS = 3
MOST_DIRECT = 64
LOW, HIGH = 2, 3
GHOSTS = (((0, 1, 2), 1, 2), ((3,), LOW, HIGH))
MESH_ID = pl.DeviceIdType.MESH
AXES = ("gx", "gy", "gz")


def round_up(value, multiple):
    return -(-value // multiple) * multiple


def axis_groups(count):
    groups = {}
    for shift in (0, -1, 1):
        groups.setdefault(shift % count, []).append(shift)
    return list(groups.items())


def span(shifts, size):
    if shifts == [0]:
        return 1, size + 3
    if shifts == [-1]:
        return 0, 4
    if shifts == [1]:
        return size + 1, 4
    return 0, size + 5


def weights(fraction):
    root = jnp.sqrt(1.0 + 4.0 * fraction - 4.0 * fraction * fraction)
    near, far = 3.0 - 2.0 * fraction, 1.0 + 2.0 * fraction
    return ((near - root) / 8.0, (near + root) / 8.0, (far + root) / 8.0, (far - root) / 8.0)


def table(cell, four, shifts, size, first, rows):
    place = lax.broadcasted_iota(jnp.int32, (rows, cell.shape[1]), 0).astype(jnp.float32) + first
    total = None
    for shift in shifts:
        apart = place - (cell + (shift * size - 1.0))
        part = jnp.where(apart == 3.0, four[3], 0.0)
        for number in (2, 1, 0):
            part = jnp.where(apart == float(number), four[number], part)
        total = part if total is None else total + part
    return total


def split(value):
    high = value.astype(jnp.bfloat16)
    return high, (value - high.astype(jnp.float32)).astype(jnp.bfloat16)


def dot_nt(a, b):
    return lax.dot_general(a, b, (((1,), (1,)), ((), ())), preferred_element_type=jnp.float32)


def dot_nn(a, b):
    return lax.dot_general(a, b, (((1,), (0,)), ((), ())), preferred_element_type=jnp.float32)


def kernel(
    counts, sizes, density_in, velocity_in, cells_in, offsets_in, target_in, stiffness_in, live_in, out,
    block, dense, cell, offset, target, stiffness, held, slab, slabs, nbuf, fbuf, rbuf, dbuf, thi, tlo, tz, tzn, wide,
    planar, grid, lsem, nsend, nrecv, rsend, rrecv, dsend, drecv, ssend, srecv, *ghosts,
):
    size_x, size_y, size_z = sizes
    cap = cell.shape[1]
    rows_y, low_z = size_y + 8, 8
    assert size_y == 8
    wide_x = size_x + 5
    tall_z, wide_xy = planar.shape[1], planar.shape[2]
    groups = [axis_groups(count) for count in counts]
    near_x, near_y, near_z = (len(group) for group in groups)
    flat = near_x * near_y
    places = sorted(
        itertools.product(range(near_x), range(near_y), range(near_z)),
        key=lambda place: (place[2] > 0, place[0], place[2], place[1]),
    )
    slots = [tuple(group[k][0] for group, k in zip(groups, place)) for place in places]
    parts = [(1, flat), (flat, len(slots))]
    me = [lax.axis_index(name) for name in AXES]
    sent = []

    def device(offset):
        return tuple(lax.rem(m + o, n) for m, o, n in zip(me, offset, counts))

    def negated(offset):
        return tuple((-o) % n for o, n in zip(offset, counts))

    peers = {slot for slot in slots if any(slot)}
    for axis, count in enumerate(counts):
        for step in range(1, count):
            peers.add(tuple(step if a == axis else 0 for a in range(3)))
    everyone = [o for o in itertools.product(*[range(n) for n in counts]) if any(o)]
    direct = len(everyone) < MOST_DIRECT
    peers = everyone if direct else sorted(peers)
    offs_y = sorted({1 % counts[1], (-1) % counts[1]})
    line = lax.broadcasted_iota(jnp.int32, (8, size_z), 0)
    wide_line = lax.broadcasted_iota(jnp.int32, (8, wide_xy), 0)

    def halo_copy(sems, number, source, target_ref, offset):
        return pltpu.make_async_remote_copy(
            src_ref=source,
            dst_ref=target_ref,
            send_sem=sems[0].at[number],
            recv_sem=sems[1].at[number],
            device_id=device(negated(offset)),
            device_id_type=MESH_ID,
        )

    def exchange(number):
        (names, low, high), (xl, xh, pack, lpack, hpack, yb, lb, hb, send, recv) = GHOSTS[number], ghosts[10 * number : 10 * number + 10]
        at, sems = pl.ds(names[0], len(names)), (send, recv)
        below, above = (-1) % counts[0], 1 % counts[0]
        copies = []
        for k, off in enumerate(offs_y):
            copies += [
                halo_copy(sems, 2 + 3 * k, pack, yb.at[k], (0, off, 0)),
                halo_copy(sems, 3 + 3 * k, lpack, lb.at[k], (below, off, 0)),
                halo_copy(sems, 4 + 3 * k, hpack, hb.at[k], (above, off, 0)),
            ]
        copies += [
            halo_copy(sems, 0, block.at[at, pl.ds(size_x - low, low)], xl, (below, 0, 0)),
            halo_copy(sems, 1, block.at[at, pl.ds(0, high)], xh, (above, 0, 0)),
        ]
        return copies

    def slab_copy(number):
        return pltpu.make_async_remote_copy(
            src_ref=slab,
            dst_ref=slabs.at[number - flat],
            send_sem=ssend.at[0],
            recv_sem=srecv.at[0],
            device_id=device(negated(slots[number])),
            device_id_type=MESH_ID,
        )

    def prepare():
        for number, (names, low, high) in enumerate(GHOSTS):
            pack, lpack, hpack = ghosts[10 * number + 2 : 10 * number + 5]
            levels = [size_y - low + j for j in range(low)] + list(range(high))
            for f, name in enumerate(names):
                for j, level in enumerate(levels):
                    kind = f * len(levels) + j
                    for q in range(size_x):
                        row = block[name, q, pl.ds(level, 1), :]
                        pack[kind, pl.ds(q, 1), :] = row
                        if q >= size_x - low:
                            lpack[pl.ds(kind * low + q - size_x + low, 1), :] = row
                        if q < high:
                            hpack[pl.ds(kind * high + q, 1), :] = row
        for pair in range(2):
            level = jnp.concatenate(
                [block[2 * pair + 1 - half, q] for q in range(size_x) for half in range(2)], axis=0
            )
            turned = jnp.transpose(level)
            slab[pair] = jnp.where(line[:, : rows_y * size_x] < HIGH, turned[:8], turned[size_z - 8 :])

    def assemble(number):
        (names, low, high), (xl, xh, pack, lpack, hpack, yb, lb, hb, send, recv) = GHOSTS[number], ghosts[10 * number : 10 * number + 10]
        kinds = low + high
        k_below, k_above = offs_y.index((-1) % counts[1]), offs_y.index(1 % counts[1])
        empty = jnp.zeros((8, size_z), jnp.float32)

        def core(f, p):
            if p < LOW:
                return xl[f, p - LOW + low] if p >= LOW - low else empty
            if p < LOW + size_x:
                return block[names[f], p - LOW]
            return xh[f, p - LOW - size_x] if p < LOW + size_x + high else empty

        def beside(f, p, j):
            k, kind = (k_below if j < low else k_above), f * kinds + j
            if LOW - low <= p < LOW:
                return lb[k, pl.ds(kind * low + p - LOW + low, 1), :]
            if LOW <= p < LOW + size_x:
                return yb[k, kind, pl.ds(p - LOW, 1), :]
            if LOW + size_x <= p < LOW + size_x + high:
                return hb[k, pl.ds(kind * high + p - LOW - size_x, 1), :]
            return None

        lane = lax.broadcasted_iota(jnp.int32, (8, wide_xy), 1) - (8 - LOW)
        plane, level = lane // rows_y, lane % rows_y
        blank = jnp.zeros((wide_xy - (wide_x + 1) * rows_y, size_z), jnp.float32)
        ends = {}
        for shift_x, shift_y in itertools.product((0, -1, 1), (0, -1, 1)):
            inside = (lane >= 0) & (plane < wide_x) & (level < size_y + LOW + HIGH)
            for value, shift, size in ((plane, shift_x, size_x), (level, shift_y, size_y)):
                inside &= (value >= LOW + shift * size) & (value < LOW + (shift + 1) * size)
            for shift_z in (-1, 1):
                offset_of = tuple(o % n for o, n in zip((shift_x, shift_y, shift_z), counts))
                got = slabs.at[slots.index(offset_of) - flat]
                for name in names:
                    by = (shift_x * size_x + LOW) * rows_y + shift_y * size_y + (0, 8)[name % 2]
                    edge = jnp.concatenate([got[name // 2], jnp.zeros((8, wide_xy - rows_y * size_x), jnp.float32)], axis=1)
                    edge = pltpu.roll(edge, by % wide_xy, 1)
                    ends[name, shift_z] = jnp.where(inside, edge, ends.get((name, shift_z), 0.0))
        for f, name in enumerate(names):
            tiles = []
            for p in range(wide_x + 1):
                ghost = empty
                for j in range(kinds):
                    row = beside(f, p, j) if j < low else beside(f, p - 1, j)
                    if row is not None:
                        ghost = jnp.where(line == (8 - low + j if j < low else j - low), row, ghost)
                tiles += [ghost, core(f, p) if p < wide_x else empty]
            planar[name, pl.ds(low_z, size_z)] = jnp.transpose(jnp.concatenate(tiles + [blank], axis=0))
            planar[name, pl.ds(0, 8)] = jnp.where(wide_line >= 8 - LOW, ends[name, -1], 0.0)
            planar[name, pl.ds(low_z + size_z, 8)] = jnp.where(wide_line < HIGH, ends[name, 1], 0.0)

    loads = [
        pltpu.make_async_copy(source, target_ref, lsem.at[number])
        for number, (source, target_ref) in enumerate((
            (density_in, dense), (velocity_in, block.at[pl.ds(0, 3)]), (cells_in, cell), (offsets_in, offset),
            (target_in, target), (stiffness_in, stiffness), (live_in, held),
        ))
    ]
    barrier = pltpu.get_barrier_semaphore()
    for peer in peers:
        pl.semaphore_signal(barrier, inc=1, device_id=device(peer), device_id_type=MESH_ID)
    for load in loads:
        load.start()
    for load in loads[:2]:
        load.wait()
    block[3] = lax.rsqrt(dense[...])
    prepare()
    for load in loads[2:]:
        load.wait()
    corner = [m * size for m, size in zip(me, sizes)]
    for k in range(3):
        nbuf[0, pl.ds(k, 1), :] = (cell[pl.ds(k, 1), :] - corner[k]).astype(jnp.float32)
    nbuf[0, pl.ds(3, 3), :] = offset[...]
    nbuf[0, pl.ds(6, 2), :] = jnp.zeros((2, cap), jnp.float32)
    live = (lax.broadcasted_iota(jnp.int32, (1, cap), 1) < held[0]).astype(jnp.float32)
    pl.semaphore_wait(barrier, len(peers))

    def neighbour_copy(turn, number):
        return pltpu.make_async_remote_copy(
            src_ref=fbuf.at[turn - 1, 0] if turn else nbuf.at[0],
            dst_ref=fbuf.at[turn - 1, number] if turn else nbuf.at[number],
            send_sem=nsend.at[min(turn, 1)],
            recv_sem=nrecv.at[turn, int(number >= flat)],
            device_id=device(negated(slots[number])),
            device_id_type=MESH_ID,
        )

    def drain(ref, sem):
        pltpu.make_async_copy(ref, ref, sem).wait()

    def send_round(turn):
        for number in sorted(range(1, len(slots)), key=lambda k: (slots[k][0] == 0, k)):
            neighbour_copy(turn, number).start()

    def wait_round(turn, part):
        first, last = parts[part]
        if first < last:
            at = pl.ds(first, last - first)
            drain(fbuf.at[turn - 1, at] if turn else nbuf.at[at], nrecv.at[turn, part])

    def sum_copy(turn, stage, step):
        axis = 2 - stage
        offset = tuple((-step) % counts[axis] if a == axis else 0 for a in range(3))
        return pltpu.make_async_remote_copy(
            src_ref=rbuf.at[turn, stage, 0],
            dst_ref=rbuf.at[turn, stage, step],
            send_sem=rsend.at[turn, stage, step - 1],
            recv_sem=rrecv.at[turn, stage, step - 1],
            device_id=device(offset),
            device_id_type=MESH_ID,
        )

    def send_sum(turn, stage, value):
        rbuf[turn, stage, 0] = value
        for step in range(1, counts[2 - stage]):
            copy = sum_copy(turn, stage, step)
            copy.start()
            sent.append(copy)

    def wait_sum(turn, stage):
        for step in range(1, counts[2 - stage]):
            sum_copy(turn, stage, step).wait_recv()
        total = rbuf[turn, stage, 0]
        for step in range(1, counts[2 - stage]):
            total = total + rbuf[turn, stage, step]
        return total

    def put(turn, vector):
        for c in range(3):
            for part in range(cap // 128):
                fbuf[turn - 1, 0, pl.ds(c * (cap // 128) + part, 1), :] = vector[
                    c : c + 1, part * 128 : part * 128 + 128
                ]

    def taken(turn, number, c):
        each = cap // 128
        return jnp.concatenate(
            [fbuf[turn - 1, number, pl.ds(c * each + part, 1), :] for part in range(each)], axis=1
        )

    def direct_copy(step, number):
        return pltpu.make_async_remote_copy(
            src_ref=dbuf.at[step, 0],
            dst_ref=dbuf.at[step, number + 1],
            send_sem=dsend.at[0],
            recv_sem=drecv.at[step],
            device_id=device(negated(everyone[number])),
            device_id_type=MESH_ID,
        )

    def send_directly(step, value):
        dbuf[step, 0] = value
        for number in range(len(everyone)):
            direct_copy(step, number).start()

    def wait_directly(step):
        drain(dbuf.at[step, pl.ds(1, len(everyone))], drecv.at[step])
        return jnp.sum(dbuf[step], axis=0)

    def reach(xi):
        start, planes = span(groups[0][xi][1], size_x)
        first = (start * rows_y + 8 - LOW) // 128 * 128
        return first, round_up((start + planes) * rows_y + HIGH, 128)

    def build(number):
        xi, yi, zi = places[number]
        info = nbuf[number]
        cells = [info[k : k + 1] for k in range(3)]
        fours = [weights(info[k + 3 : k + 4]) for k in range(3)]
        here = number * cap
        start, planes = span(groups[0][xi][1], size_x)
        tab_x = table(cells[0], fours[0], groups[0][xi][1], size_x, float(-LOW), round_up(wide_x, 8))
        shifts = groups[1][yi][1]
        side = lax.broadcasted_iota(jnp.int32, (8, cap), 0)
        tab_y = table(cells[1], fours[1], shifts, size_y, 0.0, size_y)
        below = jnp.where(side >= 8 - LOW, table(cells[1], fours[1], shifts, size_y, -8.0, 8), 0.0)
        above = jnp.where(side < HIGH, table(cells[1], fours[1], shifts, size_y, float(size_y), 8), 0.0)
        low_row, high_row = reach(xi)
        for plane in range(low_row // rows_y, high_row // rows_y):
            at = pl.ds(plane * rows_y, rows_y)
            if start <= plane < start + planes:
                mine = tab_x[plane : plane + 1]
                ghost = below * mine
                if plane > start:
                    ghost = ghost + above * tab_x[plane - 1 : plane]
                high, low = split(jnp.concatenate([ghost, tab_y * mine], axis=0))
            elif plane == start + planes:
                ghost = above * tab_x[plane - 1 : plane]
                high, low = split(jnp.concatenate([ghost, jnp.zeros_like(ghost)], axis=0))
            else:
                high = low = jnp.zeros((rows_y, cap), jnp.bfloat16)
            thi[at, pl.ds(here, cap)] = high
            tlo[at, pl.ds(here, cap)] = low
        shifts = groups[2][zi][1]
        if zi == 0:
            tz[:, pl.ds(here, cap)] = table(cells[2], fours[2], shifts, size_z, float(-low_z), tall_z)
        else:
            edge = None
            for shift in shifts:
                first = float(-LOW) if shift < 0 else size_z - 5.0
                part = table(cells[2], fours[2], [shift], size_z, first, 8)
                edge = part if edge is None else edge + part
            tzn[:, pl.ds(here - flat * cap, cap)] = edge

    def interpolate(field):
        high, low = split(field.reshape(3 * tall_z, wide_xy))
        xy_high, xy_low = thi[:, pl.ds(0, cap)], tlo[:, pl.ds(0, cap)]
        part = dot_nn(high, xy_high) + dot_nn(low, xy_high) + dot_nn(high, xy_low)
        along = tz[:, pl.ds(0, cap)]
        return jnp.concatenate(
            [
                jnp.sum(part[c * tall_z : (c + 1) * tall_z] * along, axis=0, keepdims=True)
                for c in range(3)
            ],
            axis=0,
        )

    def fill(number, rows):
        at = pl.ds(number * cap, cap)
        along = tz[:, at]
        for c in range(3):
            high, low = split(along * rows[c])
            wide[pl.ds(c * tall_z, tall_z), at] = high
            wide[pl.ds((3 + c) * tall_z, tall_z), at] = low

    def contract(xi, first, last):
        low_row, high_row = reach(xi)
        row, at = pl.ds(low_row, high_row - low_row), pl.ds(first * cap, (last - first) * cap)
        both_parts = dot_nt(wide[:, at], thi[row, at])
        half = 3 * tall_z
        return both_parts[:half] + both_parts[half:] + dot_nt(wide[pl.ds(0, half), at], tlo[row, at])

    def spread(turn, vector):
        fill(0, [vector[c : c + 1] for c in range(3)])
        own = contract(0, 0, 1)
        wait_round(turn, 0)
        for number in range(1, flat):
            fill(number, [taken(turn, number, c) for c in range(3)])
        if near_y > 1:
            own = own + contract(0, 1, near_y)
        for c in range(3):
            grid[c] = own[c * tall_z : (c + 1) * tall_z]
        for xi in range(1, near_x):
            low_row, high_row = reach(xi)
            side = contract(xi, xi * near_y, (xi + 1) * near_y)
            for c in range(3):
                grid[c, :, pl.ds(low_row, high_row - low_row)] += side[c * tall_z : (c + 1) * tall_z]
        if near_z == 1:
            return
        wait_round(turn, 1)
        each = near_y * (near_z - 1)
        for xi in range(near_x):
            low_row, high_row = reach(xi)
            row = pl.ds(low_row, high_row - low_row)
            begin = flat + xi * each
            rows = [[], [], []]
            for number in range(begin, begin + each):
                edge = tzn[:, pl.ds((number - flat) * cap, cap)]
                for c in range(3):
                    rows[c].append(edge * taken(turn, number, c))
            value = jnp.concatenate([jnp.concatenate(line, axis=1) for line in rows], axis=0)
            rounded = value.astype(jnp.bfloat16).astype(jnp.float32)
            both_parts = jnp.concatenate([rounded, value - rounded], axis=0).astype(jnp.bfloat16)
            at = pl.ds(begin * cap, each * cap)
            part = dot_nt(both_parts, thi[row, at]) + dot_nt(both_parts, tlo[row, at])
            part = part[:24] + part[24:]
            which = wide_line[:, : high_row - low_row]
            for c in range(3):
                edge = part[c * 8 : c * 8 + 8]
                early, late = pltpu.roll(edge, 6, 0), pltpu.roll(edge, 3, 0)
                grid[c, pl.ds(0, 8), row] += jnp.where(which >= 6, early, 0.0)
                grid[c, pl.ds(low_z, 8), row] += jnp.where(which < 2, early, 0.0)
                grid[c, pl.ds(size_z, 8), row] += jnp.where(which == 7, late, 0.0)
                grid[c, pl.ds(low_z + size_z, 8), row] += jnp.where(which < 3, late, 0.0)

    def shifted(value, by, axis):
        return pltpu.roll(value, by % value.shape[axis], axis)

    def both(value, axis):
        return shifted(value, -1, axis), shifted(value, 1, axis)

    def add(value, axis):
        up, down = both(value, axis)
        return up + down

    def respond():
        scale = planar[3]
        mx, my, mz = (scale * grid[c] for c in range(3))

        def along(value, step):
            return pltpu.roll(value, (-step) % wide_xy, 1)

        def paired(total, slope, step):
            return along(total + slope, step) + along(total - slope, -step)

        my_up, my_down = along(my, 1), along(my, -1)
        mz_up, mz_down = shifted(mz, -1, 0), shifted(mz, 1, 0)
        mx_up, mx_down = along(mx, rows_y), along(mx, -rows_y)
        slope_x, slope_y, slope_z = mx_up - mx_down, my_up - my_down, mz_up - mz_down
        px = paired(2.0 * mx + along(mx, 1) + along(mx, -1) + add(mx, 0), slope_y + slope_z, rows_y)
        py = paired(2.0 * my + along(my, rows_y) + along(my, -rows_y) + add(my, 0), slope_x + slope_z, 1)
        sum_z = 2.0 * mz + along(mz, 1) + along(mz, -1) + along(mz, rows_y) + along(mz, -rows_y)
        slope = slope_x + slope_y
        pz = shifted(sum_z + slope, -1, 0) + shifted(sum_z - slope, 1, 0)
        half = scale * 0.5
        return jnp.stack([half * (m + p * (1.0 / 12.0)) for m, p in ((mx, px), (my, py), (mz, pz))])

    def apply(turn, vector, summing=None):
        spread(turn, vector)
        if summing is not None:
            send_sum(summing, 1, wait_sum(summing, 0))
        field = respond()
        if summing is not None:
            send_sum(summing, 2, wait_sum(summing, 1))
        return live * (interpolate(field) + stiffness[...] * vector)

    def partial_sums(residual, image):
        folded = []
        for other in (residual, image):
            row = jnp.sum(residual * other, axis=0, keepdims=True)
            total = row[:, :128]
            for at in range(128, cap, 128):
                total = total + row[:, at : at + 128]
            folded.append(total)
        return jnp.concatenate(folded, axis=0)

    def totals(tile):
        return (
            jnp.sum(tile[0:1], axis=1, keepdims=True),
            jnp.sum(tile[1:2], axis=1, keepdims=True),
        )

    halos = [exchange(number) for number in range(2)]
    for copy in halos[0]:
        copy.start()
    for number in range(flat, len(slots)):
        slab_copy(number).start()
    send_round(0)
    for copy in halos[1]:
        copy.start()
    build(0)
    drain(slabs, srecv.at[0])
    for copy in halos[0]:
        copy.wait_recv()
    assemble(0)
    residual = live * (target[...] - interpolate(planar[pl.ds(0, 3)]))
    put(1, residual)
    send_round(1)
    for part in range(2):
        wait_round(0, part)
    for number in range(1, len(slots)):
        build(number)
    for copy in halos[1]:
        copy.wait_recv()
    assemble(1)

    image = apply(1, residual)
    direction, along, along_image = residual, image, None
    answer = None
    norm_before = alpha = None
    for step in range(ITERS):
        sums = partial_sums(residual, image)
        if step + 1 < ITERS:
            put(step + 2, image)
            send_round(step + 2)
        if direct:
            send_directly(step, sums)
            if step + 1 < ITERS:
                ahead = apply(step + 2, image)
            norm, product = totals(wait_directly(step))
        elif step + 1 < ITERS:
            send_sum(step, 0, sums)
            ahead = apply(step + 2, image, step)
            norm, product = totals(wait_sum(step, 2))
        else:
            send_sum(step, 0, sums)
            send_sum(step, 1, wait_sum(step, 0))
            send_sum(step, 2, wait_sum(step, 1))
            norm, product = totals(wait_sum(step, 2))
        if step == 0:
            alpha = norm / product
            along_image = ahead
        else:
            ratio = norm / norm_before
            alpha = norm / (product - ratio * norm / alpha)
            direction = residual + ratio * direction
            if step + 1 < ITERS:
                along = image + ratio * along
                along_image = ahead + ratio * along_image
        answer = alpha * direction if answer is None else answer + alpha * direction
        norm_before = norm
        if step + 1 < ITERS:
            residual = residual - alpha * along
            image = image - alpha * along_image
    out[...] = answer
    for copy in halos[0] + halos[1] + sent:
        copy.wait_send()
    drain(slabs, ssend.at[0])
    if len(slots) > 1:
        at = pl.ds(1, len(slots) - 1)
        drain(nbuf.at[at], nsend.at[0])
        drain(fbuf.at[:, at], nsend.at[1])
    if direct and everyone:
        drain(dbuf.at[:, pl.ds(1, len(everyone))], dsend.at[0])


def ghost_scratch(sizes, names, low, high):
    size_x, size_y, size_z = sizes
    fields, kinds = len(names), len(names) * (low + high)
    shapes = [
        (fields, low, size_y, size_z), (fields, high, size_y, size_z),
        (kinds, size_x, size_z), (kinds * low, size_z), (kinds * high, size_z),
        (2, kinds, size_x, size_z), (2, kinds * low, size_z), (2, kinds * high, size_z),
    ]
    return [pltpu.VMEM(shape, jnp.float32) for shape in shapes] + [pltpu.SemaphoreType.DMA((8,))] * 2


def body(mesh_counts, density, base_velocity, cells, offsets, target, stiffness, counts):
    sizes = density.shape
    size_x, size_y, size_z = sizes
    cap = cells.shape[1]
    rows_y = size_y + 8
    groups = [axis_groups(count) for count in mesh_counts]
    number = len(groups[0]) * len(groups[1]) * len(groups[2])
    flat = len(groups[0]) * len(groups[1])
    tall_z, wide_xy = size_z + 16, round_up((size_x + 6) * rows_y, 128)
    longest = max(mesh_counts)
    turns = ITERS + 1
    devices = mesh_counts[0] * mesh_counts[1] * mesh_counts[2]
    most = devices if devices <= MOST_DIRECT else 1
    return pl.pallas_call(
        functools.partial(kernel, mesh_counts, sizes),
        out_shape=jax.ShapeDtypeStruct((3, cap), jnp.float32),
        in_specs=[pl.BlockSpec(memory_space=pltpu.HBM)] * 7,
        out_specs=pl.BlockSpec(memory_space=pltpu.VMEM),
        scratch_shapes=[
            pltpu.VMEM((4, size_x, size_y, size_z), jnp.float32),
            pltpu.VMEM((size_x, size_y, size_z), jnp.float32),
            pltpu.VMEM((3, cap), jnp.int32),
            pltpu.VMEM((3, cap), jnp.float32),
            pltpu.VMEM((3, cap), jnp.float32),
            pltpu.VMEM((1, cap), jnp.float32),
            pltpu.SMEM((1,), jnp.int32),
            pltpu.VMEM((2, 8, rows_y * size_x), jnp.float32),
            pltpu.VMEM((number - flat, 2, 8, rows_y * size_x), jnp.float32),
            pltpu.VMEM((number, 8, cap), jnp.float32),
            pltpu.VMEM((ITERS, number, 3 * (cap // 128), 128), jnp.float32),
            pltpu.VMEM((ITERS, 3, longest, 2, 128), jnp.float32),
            pltpu.VMEM((ITERS, most, 2, 128), jnp.float32),
            pltpu.VMEM((wide_xy, number * cap), jnp.bfloat16),
            pltpu.VMEM((wide_xy, number * cap), jnp.bfloat16),
            pltpu.VMEM((tall_z, flat * cap), jnp.float32),
            pltpu.VMEM((8, max(1, len(groups[2]) - 1) * flat * cap), jnp.float32),
            pltpu.VMEM((6 * tall_z, flat * cap), jnp.bfloat16),
            pltpu.VMEM((4, tall_z, wide_xy), jnp.float32),
            pltpu.VMEM((3, tall_z, wide_xy), jnp.float32),
            pltpu.SemaphoreType.DMA((7,)),
            pltpu.SemaphoreType.DMA((2,)),
            pltpu.SemaphoreType.DMA((turns, 2)),
            pltpu.SemaphoreType.DMA((ITERS, 3, longest - 1) if most == 1 else (1, 1, 1)),
            pltpu.SemaphoreType.DMA((ITERS, 3, longest - 1) if most == 1 else (1, 1, 1)),
            pltpu.SemaphoreType.DMA((1,)),
            pltpu.SemaphoreType.DMA((ITERS,)),
            pltpu.SemaphoreType.DMA((1,)),
            pltpu.SemaphoreType.DMA((1,)),
        ] + [item for group in GHOSTS for item in ghost_scratch(sizes, *group)],
        compiler_params=pltpu.CompilerParams(
            collective_id=0, has_side_effects=True, vmem_limit_bytes=60 * 1024 * 1024
        ),
    )(density, base_velocity, cells, offsets, target, stiffness[None], counts)


def solution(mesh):
    return jax.shard_map(
        functools.partial(body, tuple(mesh.shape[name] for name in AXES)),
        mesh=mesh,
        in_specs=(
            P("gx", "gy", "gz"),
            P(None, "gx", "gy", "gz"),
            P(None, ("gx", "gy", "gz")),
            P(None, ("gx", "gy", "gz")),
            P(None, ("gx", "gy", "gz")),
            P(("gx", "gy", "gz")),
            P(("gx", "gy", "gz")),
        ),
        out_specs=P(None, ("gx", "gy", "gz")),
        check_vma=False,
    )
```

```python
import functools
import itertools

import jax
import jax.numpy as jnp
from jax import lax
from jax.experimental import pallas as pl
from jax.experimental.pallas import tpu as pltpu
from jax.sharding import PartitionSpec as P

ITERS = 3
MOST_DIRECT = 64
RESPOND_TILES = 6
LOW, HIGH = 2, 3
GHOSTS = (((0, 1, 2), 1, 2), ((3,), LOW, HIGH))
MESH_ID = pl.DeviceIdType.MESH
AXES = ("gx", "gy", "gz")


def round_up(value, multiple):
    return -(-value // multiple) * multiple


def axis_groups(count):
    groups = {}
    for shift in (0, -1, 1):
        groups.setdefault(shift % count, []).append(shift)
    return list(groups.items())


def span(shifts, size):
    if shifts == [0]:
        return 1, size + 3
    if shifts == [-1]:
        return 0, 4
    if shifts == [1]:
        return size + 1, 4
    return 0, size + 5


def weights(fraction):
    root = jnp.sqrt(1.0 + 4.0 * fraction - 4.0 * fraction * fraction)
    near, far = 3.0 - 2.0 * fraction, 1.0 + 2.0 * fraction
    return ((near - root) / 8.0, (near + root) / 8.0, (far + root) / 8.0, (far - root) / 8.0)


def table(cell, four, shifts, size, first, rows):
    place = lax.broadcasted_iota(jnp.int32, (rows, cell.shape[1]), 0).astype(jnp.float32) + first
    total = None
    for shift in shifts:
        apart = place - (cell + (shift * size - 1.0))
        part = jnp.where(apart == 3.0, four[3], 0.0)
        for number in (2, 1, 0):
            part = jnp.where(apart == float(number), four[number], part)
        total = part if total is None else total + part
    return total


def split(value):
    high = value.astype(jnp.bfloat16)
    return high, (value - high.astype(jnp.float32)).astype(jnp.bfloat16)


def dot_nt(a, b):
    return lax.dot_general(a, b, (((1,), (1,)), ((), ())), preferred_element_type=jnp.float32)


def dot_nn(a, b):
    return lax.dot_general(a, b, (((1,), (0,)), ((), ())), preferred_element_type=jnp.float32)


def kernel(
    counts, sizes, density_in, velocity_in, cells_in, offsets_in, target_in, stiffness_in, live_in, out,
    block, dense, cell, offset, target, stiffness, held, slab, slabs, nbuf, fbuf, rbuf, dbuf, thi, tlo, tz, tzn, wide,
    planar, grid, lsem, nsend, nrecv, rsend, rrecv, dsend, drecv, ssend, srecv, *ghosts,
):
    size_x, size_y, size_z = sizes
    cap = cell.shape[1]
    rows_y, low_z = size_y + 8, 8
    assert size_y == 8
    wide_x = size_x + 5
    tall_z, wide_xy = planar.shape[1], planar.shape[2]
    groups = [axis_groups(count) for count in counts]
    near_x, near_y, near_z = (len(group) for group in groups)
    flat = near_x * near_y
    places = sorted(
        itertools.product(range(near_x), range(near_y), range(near_z)),
        key=lambda place: (place[0] > 0, place[2] > 0, place[0], place[2], place[1]),
    )
    slots = [tuple(group[k][0] for group, k in zip(groups, place)) for place in places]
    each = near_y * (near_z - 1)
    middle = near_y * near_z
    parts = [(1, middle), (middle, middle + flat - near_y), (middle + flat - near_y, len(slots))]
    part_of = {number: k for k, part in enumerate(parts) for number in range(*part)}
    edges = [number for number, place in enumerate(places) if place[2]]
    farthest = sorted(range(1, len(slots)), key=lambda k: (-sum(map(bool, slots[k])), slots[k][0] == 0, k))
    me = [lax.axis_index(name) for name in AXES]
    sent = []

    def device(offset):
        return tuple(lax.rem(m + o, n) for m, o, n in zip(me, offset, counts))

    def negated(offset):
        return tuple((-o) % n for o, n in zip(offset, counts))

    peers = {slot for slot in slots if any(slot)}
    for axis, count in enumerate(counts):
        for step in range(1, count):
            peers.add(tuple(step if a == axis else 0 for a in range(3)))
    everyone = sorted(
        (o for o in itertools.product(*[range(n) for n in counts]) if any(o)),
        key=lambda offset: -sum(min(o, n - o) for o, n in zip(offset, counts)),
    )
    direct = len(everyone) < MOST_DIRECT
    peers = everyone if direct else sorted(peers)
    offs_y = sorted({1 % counts[1], (-1) % counts[1]})
    line = lax.broadcasted_iota(jnp.int32, (8, size_z), 0)
    wide_line = lax.broadcasted_iota(jnp.int32, (8, wide_xy), 0)

    def halo_copy(sems, number, source, target_ref, offset):
        return pltpu.make_async_remote_copy(
            src_ref=source,
            dst_ref=target_ref,
            send_sem=sems[0].at[number],
            recv_sem=sems[1].at[number],
            device_id=device(negated(offset)),
            device_id_type=MESH_ID,
        )

    def exchange(number):
        (names, low, high), (xl, xh, pack, lpack, hpack, yb, lb, hb, send, recv) = GHOSTS[number], ghosts[10 * number : 10 * number + 10]
        at, sems = pl.ds(names[0], len(names)), (send, recv)
        below, above = (-1) % counts[0], 1 % counts[0]
        copies = []
        for k, off in enumerate(offs_y):
            copies += [
                halo_copy(sems, 2 + 3 * k, pack, yb.at[k], (0, off, 0)),
                halo_copy(sems, 3 + 3 * k, lpack, lb.at[k], (below, off, 0)),
                halo_copy(sems, 4 + 3 * k, hpack, hb.at[k], (above, off, 0)),
            ]
        copies += [
            halo_copy(sems, 0, block.at[at, pl.ds(size_x - low, low)], xl, (below, 0, 0)),
            halo_copy(sems, 1, block.at[at, pl.ds(0, high)], xh, (above, 0, 0)),
        ]
        return copies

    def slab_copy(number):
        return pltpu.make_async_remote_copy(
            src_ref=slab,
            dst_ref=slabs.at[edges.index(number)],
            send_sem=ssend.at[0],
            recv_sem=srecv.at[0],
            device_id=device(negated(slots[number])),
            device_id_type=MESH_ID,
        )

    def prepare():
        for number, (names, low, high) in enumerate(GHOSTS):
            pack, lpack, hpack = ghosts[10 * number + 2 : 10 * number + 5]
            levels = [size_y - low + j for j in range(low)] + list(range(high))
            for f, name in enumerate(names):
                for j, level in enumerate(levels):
                    kind = f * len(levels) + j
                    for q in range(size_x):
                        row = block[name, q, pl.ds(level, 1), :]
                        pack[kind, pl.ds(q, 1), :] = row
                        if q >= size_x - low:
                            lpack[pl.ds(kind * low + q - size_x + low, 1), :] = row
                        if q < high:
                            hpack[pl.ds(kind * high + q, 1), :] = row
        for pair in range(2):
            level = jnp.concatenate(
                [block[2 * pair + 1 - half, q] for q in range(size_x) for half in range(2)], axis=0
            )
            turned = jnp.transpose(level)
            slab[pair] = jnp.where(line[:, : rows_y * size_x] < HIGH, turned[:8], turned[size_z - 8 :])

    def assemble(number):
        (names, low, high), (xl, xh, pack, lpack, hpack, yb, lb, hb, send, recv) = GHOSTS[number], ghosts[10 * number : 10 * number + 10]
        kinds = low + high
        k_below, k_above = offs_y.index((-1) % counts[1]), offs_y.index(1 % counts[1])
        empty = jnp.zeros((8, size_z), jnp.float32)

        def core(f, p):
            if p < LOW:
                return xl[f, p - LOW + low] if p >= LOW - low else empty
            if p < LOW + size_x:
                return block[names[f], p - LOW]
            return xh[f, p - LOW - size_x] if p < LOW + size_x + high else empty

        def beside(f, p, j):
            k, kind = (k_below if j < low else k_above), f * kinds + j
            if LOW - low <= p < LOW:
                return lb[k, pl.ds(kind * low + p - LOW + low, 1), :]
            if LOW <= p < LOW + size_x:
                return yb[k, kind, pl.ds(p - LOW, 1), :]
            if LOW + size_x <= p < LOW + size_x + high:
                return hb[k, pl.ds(kind * high + p - LOW - size_x, 1), :]
            return None

        lane = lax.broadcasted_iota(jnp.int32, (8, wide_xy), 1) - (8 - LOW)
        plane, level = lane // rows_y, lane % rows_y
        blank = jnp.zeros((wide_xy - (wide_x + 1) * rows_y, size_z), jnp.float32)
        ends = {}
        for shift_x, shift_y in itertools.product((0, -1, 1), (0, -1, 1)):
            inside = (lane >= 0) & (plane < wide_x) & (level < size_y + LOW + HIGH)
            for value, shift, size in ((plane, shift_x, size_x), (level, shift_y, size_y)):
                inside &= (value >= LOW + shift * size) & (value < LOW + (shift + 1) * size)
            for shift_z in (-1, 1):
                offset_of = tuple(o % n for o, n in zip((shift_x, shift_y, shift_z), counts))
                got = slabs.at[edges.index(slots.index(offset_of))]
                for name in names:
                    by = (shift_x * size_x + LOW) * rows_y + shift_y * size_y + (0, 8)[name % 2]
                    edge = jnp.concatenate([got[name // 2], jnp.zeros((8, wide_xy - rows_y * size_x), jnp.float32)], axis=1)
                    edge = pltpu.roll(edge, by % wide_xy, 1)
                    ends[name, shift_z] = jnp.where(inside, edge, ends.get((name, shift_z), 0.0))
        for f, name in enumerate(names):
            tiles = []
            for p in range(wide_x + 1):
                ghost = empty
                for j in range(kinds):
                    row = beside(f, p, j) if j < low else beside(f, p - 1, j)
                    if row is not None:
                        ghost = jnp.where(line == (8 - low + j if j < low else j - low), row, ghost)
                tiles += [ghost, core(f, p) if p < wide_x else empty]
            planar[name, pl.ds(low_z, size_z)] = jnp.transpose(jnp.concatenate(tiles + [blank], axis=0))
            planar[name, pl.ds(0, 8)] = jnp.where(wide_line >= 8 - LOW, ends[name, -1], 0.0)
            planar[name, pl.ds(low_z + size_z, 8)] = jnp.where(wide_line < HIGH, ends[name, 1], 0.0)

    loads = [
        pltpu.make_async_copy(source, target_ref, lsem.at[number])
        for number, (source, target_ref) in enumerate((
            (density_in, dense), (velocity_in, block.at[pl.ds(0, 3)]), (cells_in, cell), (offsets_in, offset),
            (target_in, target), (stiffness_in, stiffness), (live_in, held),
        ))
    ]
    barrier = pltpu.get_barrier_semaphore()
    for peer in peers:
        pl.semaphore_signal(barrier, inc=1, device_id=device(peer), device_id_type=MESH_ID)
    for load in loads:
        load.start()
    for load in loads[:2]:
        load.wait()
    block[3] = lax.rsqrt(dense[...])
    prepare()
    for load in loads[2:]:
        load.wait()
    corner = [m * size for m, size in zip(me, sizes)]
    for k in range(3):
        nbuf[0, pl.ds(k, 1), :] = (cell[pl.ds(k, 1), :] - corner[k]).astype(jnp.float32)
    nbuf[0, pl.ds(3, 3), :] = offset[...]
    nbuf[0, pl.ds(6, 2), :] = jnp.zeros((2, cap), jnp.float32)
    live = (lax.broadcasted_iota(jnp.int32, (1, cap), 1) < held[0]).astype(jnp.float32)
    pl.semaphore_wait(barrier, len(peers))

    def neighbour_copy(turn, number):
        return pltpu.make_async_remote_copy(
            src_ref=fbuf.at[turn - 1, 0] if turn else nbuf.at[0],
            dst_ref=fbuf.at[turn - 1, number] if turn else nbuf.at[number],
            send_sem=nsend.at[min(turn, 1)],
            recv_sem=nrecv.at[turn, part_of[number]],
            device_id=device(negated(slots[number])),
            device_id_type=MESH_ID,
        )

    def drain(ref, sem):
        pltpu.make_async_copy(ref, ref, sem).wait()

    def send_round(turn):
        for number in farthest:
            neighbour_copy(turn, number).start()

    def wait_round(turn, part):
        first, last = parts[part]
        if first < last:
            at = pl.ds(first, last - first)
            drain(fbuf.at[turn - 1, at] if turn else nbuf.at[at], nrecv.at[turn, part])

    def sum_copy(turn, stage, step):
        axis = 2 - stage
        offset = tuple((-step) % counts[axis] if a == axis else 0 for a in range(3))
        return pltpu.make_async_remote_copy(
            src_ref=rbuf.at[turn, stage, 0],
            dst_ref=rbuf.at[turn, stage, step],
            send_sem=rsend.at[turn, stage, step - 1],
            recv_sem=rrecv.at[turn, stage, step - 1],
            device_id=device(offset),
            device_id_type=MESH_ID,
        )

    def send_sum(turn, stage, value):
        rbuf[turn, stage, 0] = value
        for step in range(1, counts[2 - stage]):
            copy = sum_copy(turn, stage, step)
            copy.start()
            sent.append(copy)

    def wait_sum(turn, stage):
        for step in range(1, counts[2 - stage]):
            sum_copy(turn, stage, step).wait_recv()
        total = rbuf[turn, stage, 0]
        for step in range(1, counts[2 - stage]):
            total = total + rbuf[turn, stage, step]
        return total

    def put(turn, vector):
        for c in range(3):
            for part in range(cap // 128):
                fbuf[turn - 1, 0, pl.ds(c * (cap // 128) + part, 1), :] = vector[
                    c : c + 1, part * 128 : part * 128 + 128
                ]

    def taken(turn, number, c):
        each = cap // 128
        return jnp.concatenate(
            [fbuf[turn - 1, number, pl.ds(c * each + part, 1), :] for part in range(each)], axis=1
        )

    def direct_copy(step, number):
        return pltpu.make_async_remote_copy(
            src_ref=dbuf.at[step, 0],
            dst_ref=dbuf.at[step, number + 1],
            send_sem=dsend.at[0],
            recv_sem=drecv.at[step],
            device_id=device(negated(everyone[number])),
            device_id_type=MESH_ID,
        )

    def send_directly(step, value):
        dbuf[step, 0] = value
        for number in range(len(everyone)):
            direct_copy(step, number).start()

    def wait_directly(step):
        drain(dbuf.at[step, pl.ds(1, len(everyone))], drecv.at[step])
        return jnp.sum(dbuf[step], axis=0)

    def reach(xi):
        start, planes = span(groups[0][xi][1], size_x)
        first = (start * rows_y + 8 - LOW) // 128 * 128
        return first, round_up((start + planes) * rows_y + HIGH, 128)

    def build(number):
        xi, yi, zi = places[number]
        info = nbuf[number]
        cells = [info[k : k + 1] for k in range(3)]
        fours = [weights(info[k + 3 : k + 4]) for k in range(3)]
        here = number * cap
        start, planes = span(groups[0][xi][1], size_x)
        tab_x = table(cells[0], fours[0], groups[0][xi][1], size_x, float(-LOW), round_up(wide_x, 8))
        shifts = groups[1][yi][1]
        side = lax.broadcasted_iota(jnp.int32, (8, cap), 0)
        tab_y = table(cells[1], fours[1], shifts, size_y, 0.0, size_y)
        below = jnp.where(side >= 8 - LOW, table(cells[1], fours[1], shifts, size_y, -8.0, 8), 0.0)
        above = jnp.where(side < HIGH, table(cells[1], fours[1], shifts, size_y, float(size_y), 8), 0.0)
        low_row, high_row = reach(xi)
        for plane in range(low_row // rows_y, high_row // rows_y):
            at = pl.ds(plane * rows_y, rows_y)
            if start <= plane < start + planes:
                mine = tab_x[plane : plane + 1]
                ghost = below * mine
                if plane > start:
                    ghost = ghost + above * tab_x[plane - 1 : plane]
                high, low = split(jnp.concatenate([ghost, tab_y * mine], axis=0))
            elif plane == start + planes:
                ghost = above * tab_x[plane - 1 : plane]
                high, low = split(jnp.concatenate([ghost, jnp.zeros_like(ghost)], axis=0))
            else:
                high = low = jnp.zeros((rows_y, cap), jnp.bfloat16)
            thi[at, pl.ds(here, cap)] = high
            tlo[at, pl.ds(here, cap)] = low
        shifts = groups[2][zi][1]
        if zi == 0:
            tz[:, pl.ds((xi * near_y + yi) * cap, cap)] = table(cells[2], fours[2], shifts, size_z, float(-low_z), tall_z)
        else:
            edge = None
            for shift in shifts:
                first = float(-LOW) if shift < 0 else size_z - 5.0
                part = table(cells[2], fours[2], [shift], size_z, first, 8)
                edge = part if edge is None else edge + part
            tzn[:, pl.ds(edges.index(number) * cap, cap)] = edge

    def interpolate(field):
        high, low = split(field)
        xy_high, xy_low = thi[:, pl.ds(0, cap)], tlo[:, pl.ds(0, cap)]
        both_parts = dot_nn(jnp.concatenate([high, low], axis=0), xy_high)
        part = both_parts[: 3 * tall_z] + both_parts[3 * tall_z :] + dot_nn(high, xy_low)
        heights = tz[:, pl.ds(0, cap)]
        return jnp.concatenate(
            [
                jnp.sum(part[c * tall_z : (c + 1) * tall_z] * heights, axis=0, keepdims=True)
                for c in range(3)
            ],
            axis=0,
        )

    def fill(number, rows):
        xi, yi, _ = places[number]
        at = pl.ds((xi * near_y + yi) * cap, cap)
        heights = tz[:, at]
        for c in range(3):
            high, low = split(heights * rows[c])
            wide[pl.ds(c * tall_z, tall_z), at] = high
            wide[pl.ds((3 + c) * tall_z, tall_z), at] = low

    def contract(first, last):
        xi, yi, _ = places[first]
        low_row, high_row = reach(xi)
        row, count = pl.ds(low_row, high_row - low_row), (last - first) * cap
        at, here = pl.ds(first * cap, count), pl.ds((xi * near_y + yi) * cap, count)
        both_parts = dot_nt(wide[:, here], thi[row, at])
        half = 3 * tall_z
        return both_parts[:half] + both_parts[half:] + dot_nt(wide[pl.ds(0, half), here], tlo[row, at])

    def spread(turn, vector):
        fill(0, [vector[c : c + 1] for c in range(3)])
        own = contract(0, 1)
        wait_round(turn, 0)
        for number in range(1, near_y):
            fill(number, [taken(turn, number, c) for c in range(3)])
        if near_y > 1:
            own = own + contract(1, near_y)
        for c in range(3):
            grid[c] = own[c * tall_z : (c + 1) * tall_z]
        spread_edges(turn, 0)
        wait_round(turn, 1)
        for xi in range(1, near_x):
            first = middle + (xi - 1) * near_y
            for number in range(first, first + near_y):
                fill(number, [taken(turn, number, c) for c in range(3)])
            low_row, high_row = reach(xi)
            side = contract(first, first + near_y)
            for c in range(3):
                grid[c, :, pl.ds(low_row, high_row - low_row)] += side[c * tall_z : (c + 1) * tall_z]
        wait_round(turn, 2)
        for xi in range(1, near_x):
            spread_edges(turn, xi)

    def spread_edges(turn, xi):
        if each:
            low_row, high_row = reach(xi)
            row = pl.ds(low_row, high_row - low_row)
            begin = edges[xi * each]
            rows = [[], [], []]
            for number in range(begin, begin + each):
                edge = tzn[:, pl.ds(edges.index(number) * cap, cap)]
                for c in range(3):
                    rows[c].append(edge * taken(turn, number, c))
            value = jnp.concatenate([jnp.concatenate(line, axis=1) for line in rows], axis=0)
            rounded = value.astype(jnp.bfloat16).astype(jnp.float32)
            both_parts = jnp.concatenate([rounded, value - rounded], axis=0).astype(jnp.bfloat16)
            at = pl.ds(begin * cap, each * cap)
            part = dot_nt(both_parts, thi[row, at]) + dot_nt(both_parts, tlo[row, at])
            part = part[:24] + part[24:]
            which = wide_line[:, : high_row - low_row]
            for c in range(3):
                edge = part[c * 8 : c * 8 + 8]
                early, late = pltpu.roll(edge, 6, 0), pltpu.roll(edge, 3, 0)
                grid[c, pl.ds(0, 8), row] += jnp.where(which >= 6, early, 0.0)
                grid[c, pl.ds(low_z, 8), row] += jnp.where(which < 2, early, 0.0)
                grid[c, pl.ds(size_z, 8), row] += jnp.where(which == 7, late, 0.0)
                grid[c, pl.ds(low_z + size_z, 8), row] += jnp.where(which < 3, late, 0.0)

    def slide(value, step):
        return pltpu.roll(value, (-step) % wide_xy, 1)

    def respond():
        count = tall_z // 8
        scales = [planar[3, pl.ds(8 * k, 8)] for k in range(count)]
        moved = [[scales[k] * grid[c, pl.ds(8 * k, 8)] for k in range(count)] for c in range(3)]
        result = [[], [], []]

        def shifted(c, k, step):
            near = moved[c][min(max(k + step, 0), count - 1)]
            return pltpu.roll(jnp.where(wide_line == (0 if step > 0 else 7), near, moved[c][k]), (-step) % 8, 0)

        for first_tile in range(0, count, RESPOND_TILES):
            span_of = range(first_tile, min(first_tile + RESPOND_TILES, count))
            here = [jnp.concatenate([moved[c][k] for k in span_of], axis=0) for c in range(3)]
            up = [jnp.concatenate([shifted(c, k, 1) for k in span_of], axis=0) for c in range(3)]
            down = [jnp.concatenate([shifted(c, k, -1) for k in span_of], axis=0) for c in range(3)]
            (mx, my, mz), (sx, sy, sz) = here, [u + d for u, d in zip(up, down)]
            dx, dy, dz = [u - d for u, d in zip(up, down)]
            first, second = slide(mx + my, 1) + slide(mx - my, -1), slide(mx - my, 1) + slide(mx + my, -1)
            twice = 2.0 * mx + sx
            px = slide(twice + first + dz, rows_y) + slide(twice + second - dz, -rows_y)
            first, second = slide(my + mx, rows_y) + slide(my - mx, -rows_y), slide(my - mx, rows_y) + slide(my + mx, -rows_y)
            twice = 2.0 * my + sy
            py = slide(twice + first + dz, 1) + slide(twice + second - dz, -1)
            pz = 2.0 * sz + slide(sz + dx, rows_y) + slide(sz - dx, -rows_y) + slide(sz + dy, 1) + slide(sz - dy, -1)
            half = 0.5 * jnp.concatenate([scales[k] for k in span_of], axis=0)
            for c, (m, p) in enumerate(((mx, px), (my, py), (mz, pz))):
                result[c].append(half * (m + p * (1.0 / 12.0)))
        return jnp.concatenate(result[0] + result[1] + result[2], axis=0)

    def apply(turn, vector, summing=None):
        spread(turn, vector)
        if summing is not None:
            send_sum(summing, 1, wait_sum(summing, 0))
        field = respond()
        if summing is not None:
            send_sum(summing, 2, wait_sum(summing, 1))
        return live * (interpolate(field) + stiffness[...] * vector)

    def partial_sums(residual, image):
        folded = []
        for other in (residual, image):
            row = jnp.sum(residual * other, axis=0, keepdims=True)
            total = row[:, :128]
            for at in range(128, cap, 128):
                total = total + row[:, at : at + 128]
            folded.append(total)
        return jnp.concatenate(folded, axis=0)

    def totals(tile):
        return (
            jnp.sum(tile[0:1], axis=1, keepdims=True),
            jnp.sum(tile[1:2], axis=1, keepdims=True),
        )

    halos = [exchange(number) for number in range(2)]
    for copy in halos[0]:
        copy.start()
    for number in (k for k in farthest if k in edges):
        slab_copy(number).start()
    send_round(0)
    for copy in halos[1]:
        copy.start()
    build(0)
    drain(slabs, srecv.at[0])
    for copy in halos[0]:
        copy.wait_recv()
    assemble(0)
    residual = live * (target[...] - interpolate(planar[pl.ds(0, 3)].reshape(3 * tall_z, wide_xy)))
    put(1, residual)
    send_round(1)
    for part in range(3):
        wait_round(0, part)
    for number in range(1, len(slots)):
        build(number)
    for copy in halos[1]:
        copy.wait_recv()
    assemble(1)

    image = apply(1, residual)
    direction, along, along_image = residual, image, None
    answer = None
    norm_before = alpha = None
    for step in range(ITERS):
        sums = partial_sums(residual, image)
        if step + 1 < ITERS:
            put(step + 2, image)
            send_round(step + 2)
        if direct:
            send_directly(step, sums)
            if step + 1 < ITERS:
                ahead = apply(step + 2, image)
            norm, product = totals(wait_directly(step))
        elif step + 1 < ITERS:
            send_sum(step, 0, sums)
            ahead = apply(step + 2, image, step)
            norm, product = totals(wait_sum(step, 2))
        else:
            send_sum(step, 0, sums)
            send_sum(step, 1, wait_sum(step, 0))
            send_sum(step, 2, wait_sum(step, 1))
            norm, product = totals(wait_sum(step, 2))
        if step == 0:
            alpha = norm / product
            along_image = ahead
        else:
            ratio = norm / norm_before
            alpha = norm / (product - ratio * norm / alpha)
            direction = residual + ratio * direction
            if step + 1 < ITERS:
                along = image + ratio * along
                along_image = ahead + ratio * along_image
        answer = alpha * direction if answer is None else answer + alpha * direction
        norm_before = norm
        if step + 1 < ITERS:
            residual = residual - alpha * along
            image = image - alpha * along_image
    out[...] = answer
    for copy in halos[0] + halos[1] + sent:
        copy.wait_send()
    drain(slabs, ssend.at[0])
    if len(slots) > 1:
        at = pl.ds(1, len(slots) - 1)
        drain(nbuf.at[at], nsend.at[0])
        drain(fbuf.at[:, at], nsend.at[1])
    if direct and everyone:
        drain(dbuf.at[:, pl.ds(1, len(everyone))], dsend.at[0])


def ghost_scratch(sizes, names, low, high):
    size_x, size_y, size_z = sizes
    fields, kinds = len(names), len(names) * (low + high)
    shapes = [
        (fields, low, size_y, size_z), (fields, high, size_y, size_z),
        (kinds, size_x, size_z), (kinds * low, size_z), (kinds * high, size_z),
        (2, kinds, size_x, size_z), (2, kinds * low, size_z), (2, kinds * high, size_z),
    ]
    return [pltpu.VMEM(shape, jnp.float32) for shape in shapes] + [pltpu.SemaphoreType.DMA((8,))] * 2


def body(mesh_counts, density, base_velocity, cells, offsets, target, stiffness, counts):
    sizes = density.shape
    size_x, size_y, size_z = sizes
    cap = cells.shape[1]
    rows_y = size_y + 8
    groups = [axis_groups(count) for count in mesh_counts]
    number = len(groups[0]) * len(groups[1]) * len(groups[2])
    flat = len(groups[0]) * len(groups[1])
    tall_z, wide_xy = size_z + 16, round_up((size_x + 6) * rows_y, 128)
    longest = max(mesh_counts)
    turns = ITERS + 1
    devices = mesh_counts[0] * mesh_counts[1] * mesh_counts[2]
    most = devices if devices <= MOST_DIRECT else 1
    return pl.pallas_call(
        functools.partial(kernel, mesh_counts, sizes),
        out_shape=pltpu.VMEM((3, cap), jnp.float32),
        in_specs=[pl.BlockSpec(memory_space=pltpu.HBM)] * 7,
        out_specs=pl.BlockSpec(memory_space=pltpu.VMEM),
        scratch_shapes=[
            pltpu.VMEM((4, size_x, size_y, size_z), jnp.float32),
            pltpu.VMEM((size_x, size_y, size_z), jnp.float32),
            pltpu.VMEM((3, cap), jnp.int32),
            pltpu.VMEM((3, cap), jnp.float32),
            pltpu.VMEM((3, cap), jnp.float32),
            pltpu.VMEM((1, cap), jnp.float32),
            pltpu.SMEM((1,), jnp.int32),
            pltpu.VMEM((2, 8, rows_y * size_x), jnp.float32),
            pltpu.VMEM((number - flat, 2, 8, rows_y * size_x), jnp.float32),
            pltpu.VMEM((number, 8, cap), jnp.float32),
            pltpu.VMEM((ITERS, number, 3 * (cap // 128), 128), jnp.float32),
            pltpu.VMEM((ITERS, 3, longest, 2, 128), jnp.float32),
            pltpu.VMEM((ITERS, most, 2, 128), jnp.float32),
            pltpu.VMEM((wide_xy, number * cap), jnp.bfloat16),
            pltpu.VMEM((wide_xy, number * cap), jnp.bfloat16),
            pltpu.VMEM((tall_z, flat * cap), jnp.float32),
            pltpu.VMEM((8, max(1, len(groups[2]) - 1) * flat * cap), jnp.float32),
            pltpu.VMEM((6 * tall_z, flat * cap), jnp.bfloat16),
            pltpu.VMEM((4, tall_z, wide_xy), jnp.float32),
            pltpu.VMEM((3, tall_z, wide_xy), jnp.float32),
            pltpu.SemaphoreType.DMA((7,)),
            pltpu.SemaphoreType.DMA((2,)),
            pltpu.SemaphoreType.DMA((turns, 3)),
            pltpu.SemaphoreType.DMA((ITERS, 3, longest - 1) if most == 1 else (1, 1, 1)),
            pltpu.SemaphoreType.DMA((ITERS, 3, longest - 1) if most == 1 else (1, 1, 1)),
            pltpu.SemaphoreType.DMA((1,)),
            pltpu.SemaphoreType.DMA((ITERS,)),
            pltpu.SemaphoreType.DMA((1,)),
            pltpu.SemaphoreType.DMA((1,)),
        ] + [item for group in GHOSTS for item in ghost_scratch(sizes, *group)],
        compiler_params=pltpu.CompilerParams(
            collective_id=0, has_side_effects=True, vmem_limit_bytes=60 * 1024 * 1024
        ),
    )(density, base_velocity, cells, offsets, target, stiffness[None], counts)


def solution(mesh):
    return jax.shard_map(
        functools.partial(body, tuple(mesh.shape[name] for name in AXES)),
        mesh=mesh,
        in_specs=(
            P("gx", "gy", "gz"),
            P(None, "gx", "gy", "gz"),
            P(None, ("gx", "gy", "gz")),
            P(None, ("gx", "gy", "gz")),
            P(None, ("gx", "gy", "gz")),
            P(("gx", "gy", "gz")),
            P(("gx", "gy", "gz")),
        ),
        out_specs=P(None, ("gx", "gy", "gz")),
        check_vma=False,
    )
```

```python
import functools
import itertools

import jax
import jax.numpy as jnp
from jax import lax
from jax.experimental import pallas as pl
from jax.experimental.pallas import tpu as pltpu
from jax.sharding import PartitionSpec as P

ITERS = 3
MOST_DIRECT = 64
RESPOND_TILES = 9
STAGES = 3
LOW, HIGH = 2, 3
GHOSTS = (((0, 1, 2), 1, 2), ((3,), LOW, HIGH))
MESH_ID = pl.DeviceIdType.MESH
AXES = ("gx", "gy", "gz")


def round_up(value, multiple):
    return -(-value // multiple) * multiple


def axis_groups(count):
    groups = {}
    for shift in (0, -1, 1):
        groups.setdefault(shift % count, []).append(shift)
    return list(groups.items())


def span(shifts, size):
    if shifts == [0]:
        return 1, size + 3
    if shifts == [-1]:
        return 0, 4
    if shifts == [1]:
        return size + 1, 4
    return 0, size + 5


def weights(fraction):
    root = jnp.sqrt(1.0 + 4.0 * fraction - 4.0 * fraction * fraction)
    near, far = 3.0 - 2.0 * fraction, 1.0 + 2.0 * fraction
    return ((near - root) / 8.0, (near + root) / 8.0, (far + root) / 8.0, (far - root) / 8.0)


def table(cell, four, shifts, size, first, rows):
    place = lax.broadcasted_iota(jnp.int32, (rows, cell.shape[1]), 0).astype(jnp.float32) + first
    total = None
    for shift in shifts:
        apart = place - (cell + (shift * size - 1.0))
        part = jnp.where(apart == 3.0, four[3], 0.0)
        for number in (2, 1, 0):
            part = jnp.where(apart == float(number), four[number], part)
        total = part if total is None else total + part
    return total


def split(value):
    high = value.astype(jnp.bfloat16)
    return high, (value - high.astype(jnp.float32)).astype(jnp.bfloat16)


def dot_nt(a, b):
    return lax.dot_general(a, b, (((1,), (1,)), ((), ())), preferred_element_type=jnp.float32)


def dot_nn(a, b):
    return lax.dot_general(a, b, (((1,), (0,)), ((), ())), preferred_element_type=jnp.float32)


def kernel(
    counts, sizes, density_in, velocity_in, cells_in, offsets_in, target_in, stiffness_in, live_in, out,
    block, dense, cell, offset, target, stiffness, held, slab, slabs, nbuf, fbuf, rbuf, dbuf, thi, tlo, tz, tzn, wide,
    planar, grid, lsem, nsend, nrecv, rsend, rrecv, dsend, drecv, ssend, srecv, *ghosts,
):
    size_x, size_y, size_z = sizes
    cap = cell.shape[1]
    rows_y, low_z = size_y + 8, 8
    assert size_y == 8
    wide_x = size_x + 5
    tall_z, wide_xy = planar.shape[1], planar.shape[2]
    groups = [axis_groups(count) for count in counts]
    near_x, near_y, near_z = (len(group) for group in groups)
    flat = near_x * near_y

    def stage(place):
        x, y, z = place
        if z:
            return 2 if x else 0
        return 1 if x else 0

    places = sorted(
        itertools.product(range(near_x), range(near_y), range(near_z)),
        key=lambda place: (stage(place), place[2] > 0, place[0], place[2], place[1]),
    )
    slots = [tuple(group[k][0] for group, k in zip(groups, place)) for place in places]
    each = near_y * (near_z - 1)
    parts = []
    for number in range(STAGES):
        inside = [k for k, place in enumerate(places) if k and stage(place) == number]
        parts.append((inside[0], inside[-1] + 1) if inside else (0, 0))
    part_of = {number: k for k, part in enumerate(parts) for number in range(*part)}
    edges = [number for number, place in enumerate(places) if place[2]]
    farthest = sorted(range(1, len(slots)), key=lambda k: (-sum(map(bool, slots[k])), slots[k][0] == 0, k))
    me = [lax.axis_index(name) for name in AXES]
    sent = []

    def device(offset):
        return tuple(lax.rem(m + o, n) for m, o, n in zip(me, offset, counts))

    def negated(offset):
        return tuple((-o) % n for o, n in zip(offset, counts))

    peers = {slot for slot in slots if any(slot)}
    for axis, count in enumerate(counts):
        for step in range(1, count):
            peers.add(tuple(step if a == axis else 0 for a in range(3)))
    everyone = sorted(
        (o for o in itertools.product(*[range(n) for n in counts]) if any(o)),
        key=lambda offset: -sum(min(o, n - o) for o, n in zip(offset, counts)),
    )
    direct = len(everyone) < MOST_DIRECT
    peers = everyone if direct else sorted(peers)
    offs_y = sorted({1 % counts[1], (-1) % counts[1]})
    line = lax.broadcasted_iota(jnp.int32, (8, size_z), 0)
    wide_line = lax.broadcasted_iota(jnp.int32, (8, wide_xy), 0)

    def halo_copy(sems, source, target_ref, offset):
        return pltpu.make_async_remote_copy(
            src_ref=source,
            dst_ref=target_ref,
            send_sem=sems[0].at[0],
            recv_sem=sems[1].at[0],
            device_id=device(negated(offset)),
            device_id_type=MESH_ID,
        )

    def exchange(number):
        (names, low, high), (xl, xh, pack, lpack, hpack, yb, lb, hb, tally, send, recv) = GHOSTS[number], ghosts[11 * number : 11 * number + 11]
        at, sems = pl.ds(names[0], len(names)), (send, recv)
        below, above = (-1) % counts[0], 1 % counts[0]
        copies = []
        for k, off in enumerate(offs_y):
            copies += [
                halo_copy(sems, pack, yb.at[k], (0, off, 0)),
                halo_copy(sems, lpack, lb.at[k], (below, off, 0)),
                halo_copy(sems, hpack, hb.at[k], (above, off, 0)),
            ]
        copies += [
            halo_copy(sems, block.at[at, pl.ds(size_x - low, low)], xl, (below, 0, 0)),
            halo_copy(sems, block.at[at, pl.ds(0, high)], xh, (above, 0, 0)),
        ]
        return copies

    def slab_copy(number):
        return pltpu.make_async_remote_copy(
            src_ref=slab,
            dst_ref=slabs.at[edges.index(number)],
            send_sem=ssend.at[0],
            recv_sem=srecv.at[0],
            device_id=device(negated(slots[number])),
            device_id_type=MESH_ID,
        )

    def prepare():
        for number, (names, low, high) in enumerate(GHOSTS):
            pack, lpack, hpack = ghosts[11 * number + 2 : 11 * number + 5]
            levels = [size_y - low + j for j in range(low)] + list(range(high))
            for f, name in enumerate(names):
                for j, level in enumerate(levels):
                    kind = f * len(levels) + j
                    for q in range(size_x):
                        row = block[name, q, pl.ds(level, 1), :]
                        pack[kind, pl.ds(q, 1), :] = row
                        if q >= size_x - low:
                            lpack[pl.ds(kind * low + q - size_x + low, 1), :] = row
                        if q < high:
                            hpack[pl.ds(kind * high + q, 1), :] = row
        for pair in range(2):
            level = jnp.concatenate(
                [block[2 * pair + 1 - half, q] for q in range(size_x) for half in range(2)], axis=0
            )
            turned = jnp.transpose(level)
            slab[pair] = jnp.where(line[:, : rows_y * size_x] < HIGH, turned[:8], turned[size_z - 8 :])

    def assemble(number):
        (names, low, high), (xl, xh, pack, lpack, hpack, yb, lb, hb, tally, send, recv) = GHOSTS[number], ghosts[11 * number : 11 * number + 11]
        kinds = low + high
        k_below, k_above = offs_y.index((-1) % counts[1]), offs_y.index(1 % counts[1])
        empty = jnp.zeros((8, size_z), jnp.float32)

        def core(f, p):
            if p < LOW:
                return xl[f, p - LOW + low] if p >= LOW - low else empty
            if p < LOW + size_x:
                return block[names[f], p - LOW]
            return xh[f, p - LOW - size_x] if p < LOW + size_x + high else empty

        def beside(f, p, j):
            k, kind = (k_below if j < low else k_above), f * kinds + j
            if LOW - low <= p < LOW:
                return lb[k, pl.ds(kind * low + p - LOW + low, 1), :]
            if LOW <= p < LOW + size_x:
                return yb[k, kind, pl.ds(p - LOW, 1), :]
            if LOW + size_x <= p < LOW + size_x + high:
                return hb[k, pl.ds(kind * high + p - LOW - size_x, 1), :]
            return None

        lane = lax.broadcasted_iota(jnp.int32, (8, wide_xy), 1) - (8 - LOW)
        plane, level = lane // rows_y, lane % rows_y
        blank = jnp.zeros((wide_xy - (wide_x + 1) * rows_y, size_z), jnp.float32)
        ends = {}
        for shift_x, shift_y in itertools.product((0, -1, 1), (0, -1, 1)):
            inside = (lane >= 0) & (plane < wide_x) & (level < size_y + LOW + HIGH)
            for value, shift, size in ((plane, shift_x, size_x), (level, shift_y, size_y)):
                inside &= (value >= LOW + shift * size) & (value < LOW + (shift + 1) * size)
            for shift_z in (-1, 1):
                offset_of = tuple(o % n for o, n in zip((shift_x, shift_y, shift_z), counts))
                got = slabs.at[edges.index(slots.index(offset_of))]
                for name in names:
                    by = (shift_x * size_x + LOW) * rows_y + shift_y * size_y + (0, 8)[name % 2]
                    edge = jnp.concatenate([got[name // 2], jnp.zeros((8, wide_xy - rows_y * size_x), jnp.float32)], axis=1)
                    edge = pltpu.roll(edge, by % wide_xy, 1)
                    ends[name, shift_z] = jnp.where(inside, edge, ends.get((name, shift_z), 0.0))
        for f, name in enumerate(names):
            tiles = []
            for p in range(wide_x + 1):
                ghost = empty
                for j in range(kinds):
                    row = beside(f, p, j) if j < low else beside(f, p - 1, j)
                    if row is not None:
                        ghost = jnp.where(line == (8 - low + j if j < low else j - low), row, ghost)
                tiles += [ghost, core(f, p) if p < wide_x else empty]
            planar[name, pl.ds(low_z, size_z)] = jnp.transpose(jnp.concatenate(tiles + [blank], axis=0))
            planar[name, pl.ds(0, 8)] = jnp.where(wide_line >= 8 - LOW, ends[name, -1], 0.0)
            planar[name, pl.ds(low_z + size_z, 8)] = jnp.where(wide_line < HIGH, ends[name, 1], 0.0)

    loads = [
        pltpu.make_async_copy(source, target_ref, lsem.at[number])
        for number, (source, target_ref) in enumerate((
            (density_in, dense), (velocity_in, block.at[pl.ds(0, 3)]), (cells_in, cell), (offsets_in, offset),
            (target_in, target), (stiffness_in, stiffness), (live_in, held),
        ))
    ]
    barrier = pltpu.get_barrier_semaphore()
    for load in loads:
        load.start()
    for peer in peers:
        pl.semaphore_signal(barrier, inc=1, device_id=device(peer), device_id_type=MESH_ID)
    for load in loads[:2]:
        load.wait()
    block[3] = lax.rsqrt(dense[...])
    prepare()
    for load in loads[2:]:
        load.wait()
    corner = [m * size for m, size in zip(me, sizes)]
    for k in range(3):
        nbuf[0, pl.ds(k, 1), :] = (cell[pl.ds(k, 1), :] - corner[k]).astype(jnp.float32)
    nbuf[0, pl.ds(3, 3), :] = offset[...]
    nbuf[0, pl.ds(6, 2), :] = jnp.zeros((2, cap), jnp.float32)
    live = (lax.broadcasted_iota(jnp.int32, (1, cap), 1) < held[0]).astype(jnp.float32)
    pl.semaphore_wait(barrier, len(peers))

    def neighbour_copy(turn, number):
        return pltpu.make_async_remote_copy(
            src_ref=fbuf.at[turn - 1, 0] if turn else nbuf.at[0],
            dst_ref=fbuf.at[turn - 1, number] if turn else nbuf.at[number],
            send_sem=nsend.at[min(turn, 1)],
            recv_sem=nrecv.at[turn, part_of[number]],
            device_id=device(negated(slots[number])),
            device_id_type=MESH_ID,
        )

    def drain(ref, sem):
        pltpu.make_async_copy(ref, ref, sem).wait()

    def send_round(turn):
        for number in farthest:
            neighbour_copy(turn, number).start()

    def wait_round(turn, part):
        first, last = parts[part]
        if first < last:
            at = pl.ds(first, last - first)
            drain(fbuf.at[turn - 1, at] if turn else nbuf.at[at], nrecv.at[turn, part])

    def sum_copy(turn, stage, step):
        axis = 2 - stage
        offset = tuple((-step) % counts[axis] if a == axis else 0 for a in range(3))
        return pltpu.make_async_remote_copy(
            src_ref=rbuf.at[turn, stage, 0],
            dst_ref=rbuf.at[turn, stage, step],
            send_sem=rsend.at[turn, stage, step - 1],
            recv_sem=rrecv.at[turn, stage, step - 1],
            device_id=device(offset),
            device_id_type=MESH_ID,
        )

    def send_sum(turn, stage, value):
        rbuf[turn, stage, 0] = value
        for step in range(1, counts[2 - stage]):
            copy = sum_copy(turn, stage, step)
            copy.start()
            sent.append(copy)

    def wait_sum(turn, stage):
        for step in range(1, counts[2 - stage]):
            sum_copy(turn, stage, step).wait_recv()
        total = rbuf[turn, stage, 0]
        for step in range(1, counts[2 - stage]):
            total = total + rbuf[turn, stage, step]
        return total

    def put(turn, vector):
        for c in range(3):
            for part in range(cap // 128):
                fbuf[turn - 1, 0, pl.ds(c * (cap // 128) + part, 1), :] = vector[
                    c : c + 1, part * 128 : part * 128 + 128
                ]

    def taken(turn, number, c):
        each = cap // 128
        return jnp.concatenate(
            [fbuf[turn - 1, number, pl.ds(c * each + part, 1), :] for part in range(each)], axis=1
        )

    def direct_copy(step, number):
        return pltpu.make_async_remote_copy(
            src_ref=dbuf.at[step, 0],
            dst_ref=dbuf.at[step, number + 1],
            send_sem=dsend.at[0],
            recv_sem=drecv.at[step],
            device_id=device(negated(everyone[number])),
            device_id_type=MESH_ID,
        )

    def send_directly(step, value):
        dbuf[step, 0] = value
        for number in range(len(everyone)):
            direct_copy(step, number).start()

    def wait_directly(step):
        drain(dbuf.at[step, pl.ds(1, len(everyone))], drecv.at[step])
        return jnp.sum(dbuf[step], axis=0)

    def reach(xi):
        start, planes = span(groups[0][xi][1], size_x)
        first = (start * rows_y + 8 - LOW) // 128 * 128
        return first, round_up((start + planes) * rows_y + HIGH, 128)

    def build(number):
        xi, yi, zi = places[number]
        info = nbuf[number]
        cells = [info[k : k + 1] for k in range(3)]
        fours = [weights(info[k + 3 : k + 4]) for k in range(3)]
        here = number * cap
        start, planes = span(groups[0][xi][1], size_x)
        tab_x = table(cells[0], fours[0], groups[0][xi][1], size_x, float(-LOW), round_up(wide_x, 8))
        shifts = groups[1][yi][1]
        side = lax.broadcasted_iota(jnp.int32, (8, cap), 0)
        tab_y = table(cells[1], fours[1], shifts, size_y, 0.0, size_y)
        below = jnp.where(side >= 8 - LOW, table(cells[1], fours[1], shifts, size_y, -8.0, 8), 0.0)
        above = jnp.where(side < HIGH, table(cells[1], fours[1], shifts, size_y, float(size_y), 8), 0.0)
        low_row, high_row = reach(xi)
        for plane in range(low_row // rows_y, high_row // rows_y):
            at = pl.ds(plane * rows_y, rows_y)
            if start <= plane < start + planes:
                mine = tab_x[plane : plane + 1]
                ghost = below * mine
                if plane > start:
                    ghost = ghost + above * tab_x[plane - 1 : plane]
                high, low = split(jnp.concatenate([ghost, tab_y * mine], axis=0))
            elif plane == start + planes:
                ghost = above * tab_x[plane - 1 : plane]
                high, low = split(jnp.concatenate([ghost, jnp.zeros_like(ghost)], axis=0))
            else:
                high = low = jnp.zeros((rows_y, cap), jnp.bfloat16)
            thi[at, pl.ds(here, cap)] = high
            tlo[at, pl.ds(here, cap)] = low
        shifts = groups[2][zi][1]
        if zi == 0:
            tz[:, pl.ds((xi * near_y + yi) * cap, cap)] = table(cells[2], fours[2], shifts, size_z, float(-low_z), tall_z)
        else:
            edge = None
            for shift in shifts:
                first = float(-LOW) if shift < 0 else size_z - 5.0
                part = table(cells[2], fours[2], [shift], size_z, first, 8)
                edge = part if edge is None else edge + part
            tzn[:, pl.ds(edges.index(number) * cap, cap)] = edge

    def halved(rows, table_high, table_low, dot):
        count = 3 * tall_z
        middle = round_up(count // 2, 16)
        pieces = []
        for a, b in ((0, middle), (middle, count)):
            high, low = rows(a, b)
            both_parts = dot(jnp.concatenate([high, low], axis=0), table_high)
            pieces.append(both_parts[: b - a] + both_parts[b - a :] + dot(high, table_low))
        return jnp.concatenate(pieces, axis=0)

    def interpolate(field):
        high, low = split(field)
        xy_high, xy_low = thi[:, pl.ds(0, cap)], tlo[:, pl.ds(0, cap)]
        part = halved(lambda a, b: (high[a:b], low[a:b]), xy_high, xy_low, dot_nn)
        heights = tz[:, pl.ds(0, cap)]
        return jnp.concatenate(
            [
                jnp.sum(part[c * tall_z : (c + 1) * tall_z] * heights, axis=0, keepdims=True)
                for c in range(3)
            ],
            axis=0,
        )

    def fill(number, rows):
        xi, yi, _ = places[number]
        at = pl.ds((xi * near_y + yi) * cap, cap)
        heights = tz[:, at]
        for c in range(3):
            high, low = split(heights * rows[c])
            wide[pl.ds(c * tall_z, tall_z), at] = high
            wide[pl.ds((3 + c) * tall_z, tall_z), at] = low

    def contract(first, last):
        xi, yi, _ = places[first]
        low_row, high_row = reach(xi)
        row, count = pl.ds(low_row, high_row - low_row), (last - first) * cap
        at, here = pl.ds(first * cap, count), pl.ds((xi * near_y + yi) * cap, count)
        half = 3 * tall_z
        if high_row - low_row < wide_xy:
            tables = jnp.concatenate([thi[row, at], tlo[row, at]], axis=0)
            both_parts = dot_nt(wide[:, here], tables)
            both_parts = both_parts[:half] + both_parts[half:]
            return both_parts[:, : high_row - low_row] + both_parts[:, high_row - low_row :]
        both_parts = dot_nt(wide[:, here], thi[row, at])
        return both_parts[:half] + both_parts[half:] + dot_nt(wide[pl.ds(0, half), here], tlo[row, at])

    def spread(turn, vector):
        fill(0, [vector[c : c + 1] for c in range(3)])
        own = contract(0, 1)
        wait_round(turn, 0)
        for number in range(1, near_y):
            fill(number, [taken(turn, number, c) for c in range(3)])
        if near_y > 1:
            own = own + contract(1, near_y)
        for c in range(3):
            grid[c] = own[c * tall_z : (c + 1) * tall_z]
        spread_edges(turn, 0)
        spread_sides(turn, 1)
        wait_round(turn, 2)
        spread_edges(turn, *range(1, near_x))

    def spread_sides(turn, part):
        wait_round(turn, part)
        for xi in range(1, near_x):
            numbers = [number for number in range(*parts[part]) if places[number][0] == xi]
            if numbers:
                for number in numbers:
                    fill(number, [taken(turn, number, c) for c in range(3)])
                low_row, high_row = reach(xi)
                side = contract(numbers[0], numbers[-1] + 1)
                for c in range(3):
                    grid[c, :, pl.ds(low_row, high_row - low_row)] += side[c * tall_z : (c + 1) * tall_z]

    def spread_edges(turn, *near):
        if not each or not near:
            return
        total = jnp.zeros((wide_xy, 48), jnp.float32)
        for xi in near:
            start, planes = span(groups[0][xi][1], size_x)
            low_row, high_row = start * rows_y, round_up((start + planes) * rows_y + HIGH, 16)
            row = pl.ds(low_row, high_row - low_row)
            begin = edges[xi * each]
            rows = [[], [], []]
            for number in range(begin, begin + each):
                edge = tzn[:, pl.ds(edges.index(number) * cap, cap)]
                for c in range(3):
                    rows[c].append(edge * taken(turn, number, c))
            value = jnp.concatenate([jnp.concatenate(line, axis=1) for line in rows], axis=0)
            rounded = value.astype(jnp.bfloat16).astype(jnp.float32)
            both_parts = jnp.concatenate([rounded, value - rounded], axis=0).astype(jnp.bfloat16)
            at = pl.ds(begin * cap, each * cap)
            part = dot_nt(jnp.concatenate([thi[row, at], tlo[row, at]], axis=0), both_parts)
            part = part[: high_row - low_row] + part[high_row - low_row :]
            pieces = [jnp.zeros((low_row, 48), jnp.float32)] * (low_row > 0) + [part]
            pieces += [jnp.zeros((wide_xy - high_row, 48), jnp.float32)] * (high_row < wide_xy)
            total = total + jnp.concatenate(pieces, axis=0)
        turned = jnp.transpose(jnp.concatenate([total, jnp.zeros((wide_xy, 80), jnp.float32)], axis=1))
        turned = turned[:24] + turned[24:48]
        for c in range(3):
            edge = turned[c * 8 : c * 8 + 8]
            early, late = pltpu.roll(edge, 6, 0), pltpu.roll(edge, 3, 0)
            grid[c, pl.ds(0, 8)] += jnp.where(wide_line >= 6, early, 0.0)
            grid[c, pl.ds(low_z, 8)] += jnp.where(wide_line < 2, early, 0.0)
            grid[c, pl.ds(size_z, 8)] += jnp.where(wide_line == 7, late, 0.0)
            grid[c, pl.ds(low_z + size_z, 8)] += jnp.where(wide_line < 3, late, 0.0)

    def slide(value, step):
        return pltpu.roll(value, (-step) % wide_xy, 1)

    def respond():
        count = tall_z // 8
        scales = [planar[3, pl.ds(8 * k, 8)] for k in range(count)]
        moved = [[scales[k] * grid[c, pl.ds(8 * k, 8)] for k in range(count)] for c in range(3)]
        result = [[], [], []]

        def shifted(c, k, step):
            near = moved[c][min(max(k + step, 0), count - 1)]
            return pltpu.roll(jnp.where(wide_line == (0 if step > 0 else 7), near, moved[c][k]), (-step) % 8, 0)

        for first_tile in range(0, count, RESPOND_TILES):
            span_of = range(first_tile, min(first_tile + RESPOND_TILES, count))
            here = [jnp.concatenate([moved[c][k] for k in span_of], axis=0) for c in range(3)]
            up = [jnp.concatenate([shifted(c, k, 1) for k in span_of], axis=0) for c in range(3)]
            down = [jnp.concatenate([shifted(c, k, -1) for k in span_of], axis=0) for c in range(3)]
            (mx, my, mz), (sx, sy, sz) = here, [u + d for u, d in zip(up, down)]
            dx, dy, dz = [u - d for u, d in zip(up, down)]
            first, second = slide(mx + my, 1) + slide(mx - my, -1), slide(mx - my, 1) + slide(mx + my, -1)
            twice = 2.0 * mx + sx
            px = slide(twice + first + dz, rows_y) + slide(twice + second - dz, -rows_y)
            first, second = slide(my + mx, rows_y) + slide(my - mx, -rows_y), slide(my - mx, rows_y) + slide(my + mx, -rows_y)
            twice = 2.0 * my + sy
            py = slide(twice + first + dz, 1) + slide(twice + second - dz, -1)
            pz = 2.0 * sz + slide(sz + dx, rows_y) + slide(sz - dx, -rows_y) + slide(sz + dy, 1) + slide(sz - dy, -1)
            half = 0.5 * jnp.concatenate([scales[k] for k in span_of], axis=0)
            for c, (m, p) in enumerate(((mx, px), (my, py), (mz, pz))):
                result[c].append(half * (m + p * (1.0 / 12.0)))
        return jnp.concatenate(result[0] + result[1] + result[2], axis=0)

    def apply(turn, vector, summing=None):
        spread(turn, vector)
        if summing is not None:
            send_sum(summing, 1, wait_sum(summing, 0))
        field = respond()
        if summing is not None:
            send_sum(summing, 2, wait_sum(summing, 1))
        return live * (interpolate(field) + stiffness[...] * vector)

    def partial_sums(residual, image):
        folded = []
        for other in (residual, image):
            row = jnp.sum(residual * other, axis=0, keepdims=True)
            total = row[:, :128]
            for at in range(128, cap, 128):
                total = total + row[:, at : at + 128]
            folded.append(total)
        return jnp.concatenate(folded, axis=0)

    def totals(tile):
        return (
            jnp.sum(tile[0:1], axis=1, keepdims=True),
            jnp.sum(tile[1:2], axis=1, keepdims=True),
        )

    halos = [exchange(number) for number in range(2)]
    for copy in halos[0]:
        copy.start()
    for number in (k for k in farthest if k in edges):
        slab_copy(number).start()
    send_round(0)
    for copy in halos[1]:
        copy.start()
    build(0)
    drain(slabs, srecv.at[0])
    drain(ghosts[8], ghosts[10].at[0])
    assemble(0)
    residual = live * (target[...] - interpolate(planar[pl.ds(0, 3)].reshape(3 * tall_z, wide_xy)))
    put(1, residual)
    send_round(1)
    for part in range(STAGES):
        wait_round(0, part)
        for number in range(*parts[part]):
            build(number)
    drain(ghosts[19], ghosts[21].at[0])
    assemble(1)

    image = apply(1, residual)
    direction, along, along_image = residual, image, None
    answer = None
    norm_before = alpha = None
    for step in range(ITERS):
        if step + 1 < ITERS:
            put(step + 2, image)
            send_round(step + 2)
        sums = partial_sums(residual, image)
        if direct:
            send_directly(step, sums)
            if step + 1 < ITERS:
                ahead = apply(step + 2, image)
            norm, product = totals(wait_directly(step))
        elif step + 1 < ITERS:
            send_sum(step, 0, sums)
            ahead = apply(step + 2, image, step)
            norm, product = totals(wait_sum(step, 2))
        else:
            send_sum(step, 0, sums)
            send_sum(step, 1, wait_sum(step, 0))
            send_sum(step, 2, wait_sum(step, 1))
            norm, product = totals(wait_sum(step, 2))
        if step == 0:
            alpha = norm / product
            along_image = ahead
        else:
            ratio = norm / norm_before
            alpha = norm / (product - ratio * norm / alpha)
            direction = residual + ratio * direction
            if step + 1 < ITERS:
                along = image + ratio * along
                along_image = ahead + ratio * along_image
        answer = alpha * direction if answer is None else answer + alpha * direction
        norm_before = norm
        if step + 1 < ITERS:
            residual = residual - alpha * along
            image = image - alpha * along_image
    out[...] = answer
    for copy in sent:
        copy.wait_send()
    drain(ghosts[8], ghosts[9].at[0])
    drain(ghosts[19], ghosts[20].at[0])
    drain(slabs, ssend.at[0])
    if len(slots) > 1:
        at = pl.ds(1, len(slots) - 1)
        drain(nbuf.at[at], nsend.at[0])
        drain(fbuf.at[:, at], nsend.at[1])
    if direct and everyone:
        drain(dbuf.at[:, pl.ds(1, len(everyone))], dsend.at[0])


def ghost_scratch(sizes, beside, names, low, high):
    size_x, size_y, size_z = sizes
    fields, kinds = len(names), len(names) * (low + high)
    shapes = [
        (fields, low, size_y, size_z), (fields, high, size_y, size_z),
        (kinds, size_x, size_z), (kinds * low, size_z), (kinds * high, size_z),
        (beside, kinds, size_x, size_z), (beside, kinds * low, size_z), (beside, kinds * high, size_z),
        (fields * (low + high) * size_y + beside * kinds * (size_x + low + high), size_z),
    ]
    return [pltpu.VMEM(shape, jnp.float32) for shape in shapes] + [pltpu.SemaphoreType.DMA((1,))] * 2


def body(mesh_counts, density, base_velocity, cells, offsets, target, stiffness, counts):
    sizes = density.shape
    size_x, size_y, size_z = sizes
    cap = cells.shape[1]
    rows_y = size_y + 8
    groups = [axis_groups(count) for count in mesh_counts]
    number = len(groups[0]) * len(groups[1]) * len(groups[2])
    flat = len(groups[0]) * len(groups[1])
    tall_z, wide_xy = size_z + 16, round_up((size_x + 6) * rows_y, 128)
    longest = max(mesh_counts)
    turns = ITERS + 1
    devices = mesh_counts[0] * mesh_counts[1] * mesh_counts[2]
    most = devices if devices <= MOST_DIRECT else 1
    return pl.pallas_call(
        functools.partial(kernel, mesh_counts, sizes),
        out_shape=pltpu.VMEM((3, cap), jnp.float32),
        in_specs=[pl.BlockSpec(memory_space=pltpu.HBM)] * 7,
        out_specs=pl.BlockSpec(memory_space=pltpu.VMEM),
        scratch_shapes=[
            pltpu.VMEM((4, size_x, size_y, size_z), jnp.float32),
            pltpu.VMEM((size_x, size_y, size_z), jnp.float32),
            pltpu.VMEM((3, cap), jnp.int32),
            pltpu.VMEM((3, cap), jnp.float32),
            pltpu.VMEM((3, cap), jnp.float32),
            pltpu.VMEM((1, cap), jnp.float32),
            pltpu.SMEM((1,), jnp.int32),
            pltpu.VMEM((2, 8, rows_y * size_x), jnp.float32),
            pltpu.VMEM((number - flat, 2, 8, rows_y * size_x), jnp.float32),
            pltpu.VMEM((number, 8, cap), jnp.float32),
            pltpu.VMEM((ITERS, number, 3 * (cap // 128), 128), jnp.float32),
            pltpu.VMEM((ITERS, 3, longest, 2, 128), jnp.float32),
            pltpu.VMEM((ITERS, most, 2, 128), jnp.float32),
            pltpu.VMEM((wide_xy, number * cap), jnp.bfloat16),
            pltpu.VMEM((wide_xy, number * cap), jnp.bfloat16),
            pltpu.VMEM((tall_z, flat * cap), jnp.float32),
            pltpu.VMEM((8, max(1, len(groups[2]) - 1) * flat * cap), jnp.float32),
            pltpu.VMEM((6 * tall_z, flat * cap), jnp.bfloat16),
            pltpu.VMEM((4, tall_z, wide_xy), jnp.float32),
            pltpu.VMEM((3, tall_z, wide_xy), jnp.float32),
            pltpu.SemaphoreType.DMA((7,)),
            pltpu.SemaphoreType.DMA((2,)),
            pltpu.SemaphoreType.DMA((turns, STAGES)),
            pltpu.SemaphoreType.DMA((ITERS, 3, longest - 1) if most == 1 else (1, 1, 1)),
            pltpu.SemaphoreType.DMA((ITERS, 3, longest - 1) if most == 1 else (1, 1, 1)),
            pltpu.SemaphoreType.DMA((1,)),
            pltpu.SemaphoreType.DMA((ITERS,)),
            pltpu.SemaphoreType.DMA((1,)),
            pltpu.SemaphoreType.DMA((1,)),
        ] + [item for group in GHOSTS for item in ghost_scratch(sizes, len({1 % mesh_counts[1], (-1) % mesh_counts[1]}), *group)],
        compiler_params=pltpu.CompilerParams(
            collective_id=0, has_side_effects=True, vmem_limit_bytes=60 * 1024 * 1024
        ),
    )(density, base_velocity, cells, offsets, target, stiffness[None], counts)


def solution(mesh):
    return jax.shard_map(
        functools.partial(body, tuple(mesh.shape[name] for name in AXES)),
        mesh=mesh,
        in_specs=(
            P("gx", "gy", "gz"),
            P(None, "gx", "gy", "gz"),
            P(None, ("gx", "gy", "gz")),
            P(None, ("gx", "gy", "gz")),
            P(None, ("gx", "gy", "gz")),
            P(("gx", "gy", "gz")),
            P(("gx", "gy", "gz")),
        ),
        out_specs=P(None, ("gx", "gy", "gz")),
        check_vma=False,
    )
```

```python
import functools
import itertools

import jax
import jax.numpy as jnp
from jax import lax
from jax.experimental import pallas as pl
from jax.experimental.pallas import tpu as pltpu
from jax.sharding import PartitionSpec as P

ITERS = 3
MOST_DIRECT = 64
RESPOND_TILES = 9
STAGES = 3
LOW, HIGH = 2, 3
GHOSTS = (((0, 1, 2), 1, 2), ((3,), LOW, HIGH))
MESH_ID = pl.DeviceIdType.MESH
AXES = ("gx", "gy", "gz")


def round_up(value, multiple):
    return -(-value // multiple) * multiple


def axis_groups(count):
    groups = {}
    for shift in (0, -1, 1):
        groups.setdefault(shift % count, []).append(shift)
    return list(groups.items())


def span(shifts, size):
    if shifts == [0]:
        return 1, size + 3
    if shifts == [-1]:
        return 0, 4
    if shifts == [1]:
        return size + 1, 4
    return 0, size + 5


def weights(fraction):
    root = jnp.sqrt(1.0 + 4.0 * fraction - 4.0 * fraction * fraction)
    near, far = 3.0 - 2.0 * fraction, 1.0 + 2.0 * fraction
    return ((near - root) / 8.0, (near + root) / 8.0, (far + root) / 8.0, (far - root) / 8.0)


def table(cell, four, shifts, size, first, rows):
    place = lax.broadcasted_iota(jnp.int32, (rows, cell.shape[1]), 0).astype(jnp.float32) + first
    total = None
    for shift in shifts:
        apart = place - (cell + (shift * size - 1.0))
        part = jnp.where(apart == 3.0, four[3], 0.0)
        for number in (2, 1, 0):
            part = jnp.where(apart == float(number), four[number], part)
        total = part if total is None else total + part
    return total


def split(value):
    high = value.astype(jnp.bfloat16)
    return high, (value - high.astype(jnp.float32)).astype(jnp.bfloat16)


def dot_nt(a, b):
    return lax.dot_general(a, b, (((1,), (1,)), ((), ())), preferred_element_type=jnp.float32)


def dot_nn(a, b):
    return lax.dot_general(a, b, (((1,), (0,)), ((), ())), preferred_element_type=jnp.float32)


def kernel(
    counts, sizes, density_in, velocity_in, cells_in, offsets_in, target_in, stiffness_in, live_in, out,
    block, dense, cell, offset, target, stiffness, held, slab, slabs, nbuf, fbuf, rbuf, dbuf, thi, tlo, tz, tzn, wide,
    planar, grid, lsem, nsend, nrecv, rsend, rrecv, dsend, drecv, ssend, srecv, *ghosts,
):
    size_x, size_y, size_z = sizes
    cap = cell.shape[1]
    rows_y, low_z = size_y + 8, 8
    assert size_y == 8
    wide_x = size_x + 5
    tall_z, wide_xy = planar.shape[1], planar.shape[2]
    groups = [axis_groups(count) for count in counts]
    near_x, near_y, near_z = (len(group) for group in groups)
    flat = near_x * near_y

    def stage(place):
        x, y, z = place
        if z:
            return 2 if x else 0
        return 1 if x else 0

    places = sorted(
        itertools.product(range(near_x), range(near_y), range(near_z)),
        key=lambda place: (stage(place), place[2] > 0, place[0], place[2], place[1]),
    )
    slots = [tuple(group[k][0] for group, k in zip(groups, place)) for place in places]
    each = near_y * (near_z - 1)
    parts = []
    for number in range(STAGES):
        inside = [k for k, place in enumerate(places) if k and stage(place) == number]
        parts.append((inside[0], inside[-1] + 1) if inside else (0, 0))
    part_of = {number: k for k, part in enumerate(parts) for number in range(*part)}
    edges = [number for number, place in enumerate(places) if place[2]]
    farthest = sorted(range(1, len(slots)), key=lambda k: (-sum(map(bool, slots[k])), slots[k][0] == 0, k))
    me = [lax.axis_index(name) for name in AXES]
    sent = []

    def device(offset):
        return tuple(lax.rem(m + o, n) for m, o, n in zip(me, offset, counts))

    def negated(offset):
        return tuple((-o) % n for o, n in zip(offset, counts))

    peers = {slot for slot in slots if any(slot)}
    for axis, count in enumerate(counts):
        for step in range(1, count):
            peers.add(tuple(step if a == axis else 0 for a in range(3)))
    everyone = sorted(
        (o for o in itertools.product(*[range(n) for n in counts]) if any(o)),
        key=lambda offset: -sum(min(o, n - o) for o, n in zip(offset, counts)),
    )
    direct = len(everyone) < MOST_DIRECT
    peers = everyone if direct else sorted(peers)
    offs_y = sorted({1 % counts[1], (-1) % counts[1]})
    line = lax.broadcasted_iota(jnp.int32, (8, size_z), 0)
    wide_line = lax.broadcasted_iota(jnp.int32, (8, wide_xy), 0)

    def halo_copy(sems, source, target_ref, offset):
        return pltpu.make_async_remote_copy(
            src_ref=source,
            dst_ref=target_ref,
            send_sem=sems[0].at[0],
            recv_sem=sems[1].at[0],
            device_id=device(negated(offset)),
            device_id_type=MESH_ID,
        )

    def exchange(number):
        (names, low, high), (xl, xh, pack, lpack, hpack, yb, lb, hb, tally, send, recv) = GHOSTS[number], ghosts[11 * number : 11 * number + 11]
        at, sems = pl.ds(names[0], len(names)), (send, recv)
        below, above = (-1) % counts[0], 1 % counts[0]
        copies = []
        for k, off in enumerate(offs_y):
            copies += [
                halo_copy(sems, pack, yb.at[k], (0, off, 0)),
                halo_copy(sems, lpack, lb.at[k], (below, off, 0)),
                halo_copy(sems, hpack, hb.at[k], (above, off, 0)),
            ]
        copies += [
            halo_copy(sems, block.at[at, pl.ds(size_x - low, low)], xl, (below, 0, 0)),
            halo_copy(sems, block.at[at, pl.ds(0, high)], xh, (above, 0, 0)),
        ]
        return copies

    def slab_copy(number):
        return pltpu.make_async_remote_copy(
            src_ref=slab,
            dst_ref=slabs.at[edges.index(number)],
            send_sem=ssend.at[0],
            recv_sem=srecv.at[0],
            device_id=device(negated(slots[number])),
            device_id_type=MESH_ID,
        )

    def prepare():
        for number, (names, low, high) in enumerate(GHOSTS):
            pack, lpack, hpack = ghosts[11 * number + 2 : 11 * number + 5]
            levels = [size_y - low + j for j in range(low)] + list(range(high))
            for f, name in enumerate(names):
                for j, level in enumerate(levels):
                    kind = f * len(levels) + j
                    for q in range(size_x):
                        row = block[name, q, pl.ds(level, 1), :]
                        pack[kind, pl.ds(q, 1), :] = row
                        if q >= size_x - low:
                            lpack[pl.ds(kind * low + q - size_x + low, 1), :] = row
                        if q < high:
                            hpack[pl.ds(kind * high + q, 1), :] = row
        for pair in range(2):
            level = jnp.concatenate(
                [block[2 * pair + 1 - half, q] for q in range(size_x) for half in range(2)], axis=0
            )
            turned = jnp.transpose(level)
            slab[pair] = jnp.where(line[:, : rows_y * size_x] < HIGH, turned[:8], turned[size_z - 8 :])

    def ends_of(number):
        names = GHOSTS[number][0]
        lane = lax.broadcasted_iota(jnp.int32, (8, wide_xy), 1) - (8 - LOW)
        plane, level = lane // rows_y, lane % rows_y
        ends = {}
        for shift_x, shift_y in itertools.product((0, -1, 1), (0, -1, 1)):
            inside = (lane >= 0) & (plane < wide_x) & (level < size_y + LOW + HIGH)
            for value, shift, size in ((plane, shift_x, size_x), (level, shift_y, size_y)):
                inside &= (value >= LOW + shift * size) & (value < LOW + (shift + 1) * size)
            for shift_z in (-1, 1):
                offset_of = tuple(o % n for o, n in zip((shift_x, shift_y, shift_z), counts))
                got = slabs.at[edges.index(slots.index(offset_of))]
                for name in names:
                    by = (shift_x * size_x + LOW) * rows_y + shift_y * size_y + (0, 8)[name % 2]
                    edge = jnp.concatenate([got[name // 2], jnp.zeros((8, wide_xy - rows_y * size_x), jnp.float32)], axis=1)
                    edge = pltpu.roll(edge, by % wide_xy, 1)
                    ends[name, shift_z] = jnp.where(inside, edge, ends.get((name, shift_z), 0.0))
        return [
            (jnp.where(wide_line >= 8 - LOW, ends[name, -1], 0.0), jnp.where(wide_line < HIGH, ends[name, 1], 0.0))
            for name in names
        ]

    def assemble(number, ends):
        (names, low, high), (xl, xh, pack, lpack, hpack, yb, lb, hb, tally, send, recv) = GHOSTS[number], ghosts[11 * number : 11 * number + 11]
        kinds = low + high
        k_below, k_above = offs_y.index((-1) % counts[1]), offs_y.index(1 % counts[1])
        empty = jnp.zeros((8, size_z), jnp.float32)

        def core(f, p):
            if p < LOW:
                return xl[f, p - LOW + low] if p >= LOW - low else empty
            if p < LOW + size_x:
                return block[names[f], p - LOW]
            return xh[f, p - LOW - size_x] if p < LOW + size_x + high else empty

        def beside(f, p, j):
            k, kind = (k_below if j < low else k_above), f * kinds + j
            if LOW - low <= p < LOW:
                return lb[k, pl.ds(kind * low + p - LOW + low, 1), :]
            if LOW <= p < LOW + size_x:
                return yb[k, kind, pl.ds(p - LOW, 1), :]
            if LOW + size_x <= p < LOW + size_x + high:
                return hb[k, pl.ds(kind * high + p - LOW - size_x, 1), :]
            return None

        blank = jnp.zeros((wide_xy - (wide_x + 1) * rows_y, size_z), jnp.float32)
        for f, name in enumerate(names):
            tiles = []
            for p in range(wide_x + 1):
                ghost = empty
                for j in range(kinds):
                    row = beside(f, p, j) if j < low else beside(f, p - 1, j)
                    if row is not None:
                        ghost = jnp.where(line == (8 - low + j if j < low else j - low), row, ghost)
                tiles += [ghost, core(f, p) if p < wide_x else empty]
            planar[name, pl.ds(low_z, size_z)] = jnp.transpose(jnp.concatenate(tiles + [blank], axis=0))
            planar[name, pl.ds(0, 8)] = ends[f][0] if ends else jnp.zeros((8, wide_xy), jnp.float32)
            planar[name, pl.ds(low_z + size_z, 8)] = ends[f][1] if ends else jnp.zeros((8, wide_xy), jnp.float32)

    loads = [
        pltpu.make_async_copy(source, target_ref, lsem.at[number])
        for number, (source, target_ref) in enumerate((
            (density_in, dense), (velocity_in, block.at[pl.ds(0, 3)]), (cells_in, cell), (offsets_in, offset),
            (target_in, target), (stiffness_in, stiffness), (live_in, held),
        ))
    ]
    barrier = pltpu.get_barrier_semaphore()
    for load in loads:
        load.start()
    for peer in peers:
        pl.semaphore_signal(barrier, inc=1, device_id=device(peer), device_id_type=MESH_ID)
    for load in loads[:2]:
        load.wait()
    block[3] = lax.rsqrt(dense[...])
    prepare()
    for load in loads[2:]:
        load.wait()
    corner = [m * size for m, size in zip(me, sizes)]
    for k in range(3):
        nbuf[0, pl.ds(k, 1), :] = (cell[pl.ds(k, 1), :] - corner[k]).astype(jnp.float32)
    nbuf[0, pl.ds(3, 3), :] = offset[...]
    nbuf[0, pl.ds(6, 2), :] = jnp.zeros((2, cap), jnp.float32)
    live = (lax.broadcasted_iota(jnp.int32, (1, cap), 1) < held[0]).astype(jnp.float32)
    pl.semaphore_wait(barrier, len(peers))

    def neighbour_copy(turn, number):
        return pltpu.make_async_remote_copy(
            src_ref=fbuf.at[turn - 1, 0] if turn else nbuf.at[0],
            dst_ref=fbuf.at[turn - 1, number] if turn else nbuf.at[number],
            send_sem=nsend.at[min(turn, 1)],
            recv_sem=nrecv.at[turn, part_of[number]],
            device_id=device(negated(slots[number])),
            device_id_type=MESH_ID,
        )

    def drain(ref, sem):
        pltpu.make_async_copy(ref, ref, sem).wait()

    def send_round(turn):
        for number in farthest:
            neighbour_copy(turn, number).start()

    def wait_round(turn, part):
        first, last = parts[part]
        if first < last:
            at = pl.ds(first, last - first)
            drain(fbuf.at[turn - 1, at] if turn else nbuf.at[at], nrecv.at[turn, part])

    def sum_copy(turn, stage, step):
        axis = 2 - stage
        offset = tuple((-step) % counts[axis] if a == axis else 0 for a in range(3))
        return pltpu.make_async_remote_copy(
            src_ref=rbuf.at[turn, stage, 0],
            dst_ref=rbuf.at[turn, stage, step],
            send_sem=rsend.at[turn, stage, step - 1],
            recv_sem=rrecv.at[turn, stage, step - 1],
            device_id=device(offset),
            device_id_type=MESH_ID,
        )

    def send_sum(turn, stage, value):
        rbuf[turn, stage, 0] = value
        for step in range(1, counts[2 - stage]):
            copy = sum_copy(turn, stage, step)
            copy.start()
            sent.append(copy)

    def wait_sum(turn, stage):
        for step in range(1, counts[2 - stage]):
            sum_copy(turn, stage, step).wait_recv()
        total = rbuf[turn, stage, 0]
        for step in range(1, counts[2 - stage]):
            total = total + rbuf[turn, stage, step]
        return total

    def put(turn, vector):
        for c in range(3):
            for part in range(cap // 128):
                fbuf[turn - 1, 0, pl.ds(c * (cap // 128) + part, 1), :] = vector[
                    c : c + 1, part * 128 : part * 128 + 128
                ]

    def taken(turn, number, c):
        each = cap // 128
        return jnp.concatenate(
            [fbuf[turn - 1, number, pl.ds(c * each + part, 1), :] for part in range(each)], axis=1
        )

    def direct_copy(step, number):
        return pltpu.make_async_remote_copy(
            src_ref=dbuf.at[step, 0],
            dst_ref=dbuf.at[step, number + 1],
            send_sem=dsend.at[0],
            recv_sem=drecv.at[step],
            device_id=device(negated(everyone[number])),
            device_id_type=MESH_ID,
        )

    def send_directly(step, value):
        dbuf[step, 0] = value
        for number in range(len(everyone)):
            direct_copy(step, number).start()

    def wait_directly(step):
        drain(dbuf.at[step, pl.ds(1, len(everyone))], drecv.at[step])
        return jnp.sum(dbuf[step], axis=0)

    def reach(xi):
        start, planes = span(groups[0][xi][1], size_x)
        first = (start * rows_y + 8 - LOW) // 128 * 128
        return first, round_up((start + planes) * rows_y + HIGH, 128)

    def build(number):
        xi, yi, zi = places[number]
        info = nbuf[number]
        cells = [info[k : k + 1] for k in range(3)]
        fours = [weights(info[k + 3 : k + 4]) for k in range(3)]
        here = number * cap
        start, planes = span(groups[0][xi][1], size_x)
        tab_x = table(cells[0], fours[0], groups[0][xi][1], size_x, float(-LOW), round_up(wide_x, 8))
        shifts = groups[1][yi][1]
        side = lax.broadcasted_iota(jnp.int32, (8, cap), 0)
        tab_y = table(cells[1], fours[1], shifts, size_y, 0.0, size_y)
        below = jnp.where(side >= 8 - LOW, table(cells[1], fours[1], shifts, size_y, -8.0, 8), 0.0)
        above = jnp.where(side < HIGH, table(cells[1], fours[1], shifts, size_y, float(size_y), 8), 0.0)
        low_row, high_row = reach(xi)
        for plane in range(low_row // rows_y, high_row // rows_y):
            at = pl.ds(plane * rows_y, rows_y)
            if start <= plane < start + planes:
                mine = tab_x[plane : plane + 1]
                ghost = below * mine
                if plane > start:
                    ghost = ghost + above * tab_x[plane - 1 : plane]
                high, low = split(jnp.concatenate([ghost, tab_y * mine], axis=0))
            elif plane == start + planes:
                ghost = above * tab_x[plane - 1 : plane]
                high, low = split(jnp.concatenate([ghost, jnp.zeros_like(ghost)], axis=0))
            else:
                high = low = jnp.zeros((rows_y, cap), jnp.bfloat16)
            thi[at, pl.ds(here, cap)] = high
            tlo[at, pl.ds(here, cap)] = low
        shifts = groups[2][zi][1]
        if zi == 0:
            tz[:, pl.ds((xi * near_y + yi) * cap, cap)] = table(cells[2], fours[2], shifts, size_z, float(-low_z), tall_z)
        else:
            edge = None
            for shift in shifts:
                first = float(-LOW) if shift < 0 else size_z - 5.0
                part = table(cells[2], fours[2], [shift], size_z, first, 8)
                edge = part if edge is None else edge + part
            tzn[:, pl.ds(edges.index(number) * cap, cap)] = edge

    def halved(rows, table_high, table_low, dot):
        count = 3 * tall_z
        middle = round_up(count // 2, 16)
        pieces = []
        for a, b in ((0, middle), (middle, count)):
            high, low = rows(a, b)
            both_parts = dot(jnp.concatenate([high, low], axis=0), table_high)
            pieces.append(both_parts[: b - a] + both_parts[b - a :] + dot(high, table_low))
        return jnp.concatenate(pieces, axis=0)

    def interpolate(field):
        high, low = split(field)
        xy_high, xy_low = thi[:, pl.ds(0, cap)], tlo[:, pl.ds(0, cap)]
        part = halved(lambda a, b: (high[a:b], low[a:b]), xy_high, xy_low, dot_nn)
        heights = tz[:, pl.ds(0, cap)]
        return jnp.concatenate(
            [
                jnp.sum(part[c * tall_z : (c + 1) * tall_z] * heights, axis=0, keepdims=True)
                for c in range(3)
            ],
            axis=0,
        )

    def interpolate_ends(field):
        high, low = split(field)
        xy_high, xy_low = thi[:, pl.ds(0, cap)], tlo[:, pl.ds(0, cap)]
        both_parts = jnp.concatenate([high, low], axis=0)
        part = dot_nn(both_parts, xy_high) + dot_nn(both_parts, xy_low)
        part = part[:48] + part[48:]
        heights = jnp.concatenate([tz[pl.ds(0, 8), pl.ds(0, cap)], tz[pl.ds(low_z + size_z, 8), pl.ds(0, cap)]], axis=0)
        return jnp.concatenate(
            [jnp.sum(part[16 * c : 16 * c + 16] * heights, axis=0, keepdims=True) for c in range(3)], axis=0
        )

    def fill(number, rows):
        xi, yi, _ = places[number]
        at = pl.ds((xi * near_y + yi) * cap, cap)
        heights = tz[:, at]
        for c in range(3):
            high, low = split(heights * rows[c])
            wide[pl.ds(c * tall_z, tall_z), at] = high
            wide[pl.ds((3 + c) * tall_z, tall_z), at] = low

    def contract(first, last):
        xi, yi, _ = places[first]
        low_row, high_row = reach(xi)
        row, count = pl.ds(low_row, high_row - low_row), (last - first) * cap
        at, here = pl.ds(first * cap, count), pl.ds((xi * near_y + yi) * cap, count)
        half = 3 * tall_z
        if high_row - low_row < wide_xy:
            tables = jnp.concatenate([thi[row, at], tlo[row, at]], axis=0)
            both_parts = dot_nt(wide[:, here], tables)
            both_parts = both_parts[:half] + both_parts[half:]
            return both_parts[:, : high_row - low_row] + both_parts[:, high_row - low_row :]
        both_parts = dot_nt(wide[:, here], thi[row, at])
        return both_parts[:half] + both_parts[half:] + dot_nt(wide[pl.ds(0, half), here], tlo[row, at])

    def spread(turn, vector):
        fill(0, [vector[c : c + 1] for c in range(3)])
        own = contract(0, 1)
        wait_round(turn, 0)
        for number in range(1, near_y):
            fill(number, [taken(turn, number, c) for c in range(3)])
        if near_y > 1:
            own = own + contract(1, near_y)
        for c in range(3):
            grid[c] = own[c * tall_z : (c + 1) * tall_z]
        spread_edges(turn, 0)
        spread_sides(turn, 1)
        wait_round(turn, 2)
        spread_edges(turn, *range(1, near_x))

    def spread_sides(turn, part):
        wait_round(turn, part)
        for xi in range(1, near_x):
            numbers = [number for number in range(*parts[part]) if places[number][0] == xi]
            if numbers:
                for number in numbers:
                    fill(number, [taken(turn, number, c) for c in range(3)])
                low_row, high_row = reach(xi)
                side = contract(numbers[0], numbers[-1] + 1)
                for c in range(3):
                    grid[c, :, pl.ds(low_row, high_row - low_row)] += side[c * tall_z : (c + 1) * tall_z]

    def spread_edges(turn, *near):
        if not each or not near:
            return
        total = jnp.zeros((wide_xy, 48), jnp.float32)
        for xi in near:
            start, planes = span(groups[0][xi][1], size_x)
            low_row, high_row = start * rows_y, round_up((start + planes) * rows_y + HIGH, 16)
            row = pl.ds(low_row, high_row - low_row)
            begin = edges[xi * each]
            rows = [[], [], []]
            for number in range(begin, begin + each):
                edge = tzn[:, pl.ds(edges.index(number) * cap, cap)]
                for c in range(3):
                    rows[c].append(edge * taken(turn, number, c))
            value = jnp.concatenate([jnp.concatenate(line, axis=1) for line in rows], axis=0)
            rounded = value.astype(jnp.bfloat16).astype(jnp.float32)
            both_parts = jnp.concatenate([rounded, value - rounded], axis=0).astype(jnp.bfloat16)
            at = pl.ds(begin * cap, each * cap)
            part = dot_nt(jnp.concatenate([thi[row, at], tlo[row, at]], axis=0), both_parts)
            part = part[: high_row - low_row] + part[high_row - low_row :]
            pieces = [jnp.zeros((low_row, 48), jnp.float32)] * (low_row > 0) + [part]
            pieces += [jnp.zeros((wide_xy - high_row, 48), jnp.float32)] * (high_row < wide_xy)
            total = total + jnp.concatenate(pieces, axis=0)
        turned = jnp.transpose(jnp.concatenate([total, jnp.zeros((wide_xy, 80), jnp.float32)], axis=1))
        turned = turned[:24] + turned[24:48]
        for c in range(3):
            edge = turned[c * 8 : c * 8 + 8]
            early, late = pltpu.roll(edge, 6, 0), pltpu.roll(edge, 3, 0)
            grid[c, pl.ds(0, 8)] += jnp.where(wide_line >= 6, early, 0.0)
            grid[c, pl.ds(low_z, 8)] += jnp.where(wide_line < 2, early, 0.0)
            grid[c, pl.ds(size_z, 8)] += jnp.where(wide_line == 7, late, 0.0)
            grid[c, pl.ds(low_z + size_z, 8)] += jnp.where(wide_line < 3, late, 0.0)

    def slide(value, step):
        return pltpu.roll(value, (-step) % wide_xy, 1)

    def respond():
        count = tall_z // 8
        scales = [planar[3, pl.ds(8 * k, 8)] for k in range(count)]
        moved = [[scales[k] * grid[c, pl.ds(8 * k, 8)] for k in range(count)] for c in range(3)]
        result = [[], [], []]

        def shifted(c, k, step):
            near = moved[c][min(max(k + step, 0), count - 1)]
            return pltpu.roll(jnp.where(wide_line == (0 if step > 0 else 7), near, moved[c][k]), (-step) % 8, 0)

        for first_tile in range(0, count, RESPOND_TILES):
            span_of = range(first_tile, min(first_tile + RESPOND_TILES, count))
            here = [jnp.concatenate([moved[c][k] for k in span_of], axis=0) for c in range(3)]
            up = [jnp.concatenate([shifted(c, k, 1) for k in span_of], axis=0) for c in range(3)]
            down = [jnp.concatenate([shifted(c, k, -1) for k in span_of], axis=0) for c in range(3)]
            (mx, my, mz), (sx, sy, sz) = here, [u + d for u, d in zip(up, down)]
            dx, dy, dz = [u - d for u, d in zip(up, down)]
            first, second = slide(mx + my, 1) + slide(mx - my, -1), slide(mx - my, 1) + slide(mx + my, -1)
            twice = 2.0 * mx + sx
            px = slide(twice + first + dz, rows_y) + slide(twice + second - dz, -rows_y)
            first, second = slide(my + mx, rows_y) + slide(my - mx, -rows_y), slide(my - mx, rows_y) + slide(my + mx, -rows_y)
            twice = 2.0 * my + sy
            py = slide(twice + first + dz, 1) + slide(twice + second - dz, -1)
            pz = 2.0 * sz + slide(sz + dx, rows_y) + slide(sz - dx, -rows_y) + slide(sz + dy, 1) + slide(sz - dy, -1)
            half = 0.5 * jnp.concatenate([scales[k] for k in span_of], axis=0)
            for c, (m, p) in enumerate(((mx, px), (my, py), (mz, pz))):
                result[c].append(half * (m + p * (1.0 / 12.0)))
        return jnp.concatenate(result[0] + result[1] + result[2], axis=0)

    def apply(turn, vector, summing=None):
        spread(turn, vector)
        if summing is not None:
            send_sum(summing, 1, wait_sum(summing, 0))
        field = respond()
        if summing is not None:
            send_sum(summing, 2, wait_sum(summing, 1))
        return live * (interpolate(field) + stiffness[...] * vector)

    def partial_sums(residual, image):
        folded = []
        for other in (residual, image):
            row = jnp.sum(residual * other, axis=0, keepdims=True)
            total = row[:, :128]
            for at in range(128, cap, 128):
                total = total + row[:, at : at + 128]
            folded.append(total)
        return jnp.concatenate(folded, axis=0)

    def totals(tile):
        return (
            jnp.sum(tile[0:1], axis=1, keepdims=True),
            jnp.sum(tile[1:2], axis=1, keepdims=True),
        )

    halos = [exchange(number) for number in range(2)]
    for copy in halos[0]:
        copy.start()
    for number in (k for k in farthest if k in edges):
        slab_copy(number).start()
    send_round(0)
    for copy in halos[1]:
        copy.start()
    build(0)
    drain(ghosts[8], ghosts[10].at[0])
    assemble(0, None)
    inner = interpolate(planar[pl.ds(0, 3)].reshape(3 * tall_z, wide_xy))
    drain(slabs, srecv.at[0])
    outer = interpolate_ends(jnp.concatenate([end for pair in ends_of(0) for end in pair], axis=0))
    residual = live * (target[...] - (inner + outer))
    put(1, residual)
    send_round(1)
    for part in range(STAGES):
        wait_round(0, part)
        for number in range(*parts[part]):
            build(number)
    drain(ghosts[19], ghosts[21].at[0])
    assemble(1, ends_of(1))

    image = apply(1, residual)
    direction, along, along_image = residual, image, None
    answer = None
    norm_before = alpha = None
    for step in range(ITERS):
        if step + 1 < ITERS:
            put(step + 2, image)
            send_round(step + 2)
        sums = partial_sums(residual, image)
        if direct:
            send_directly(step, sums)
            if step + 1 < ITERS:
                ahead = apply(step + 2, image)
            norm, product = totals(wait_directly(step))
        elif step + 1 < ITERS:
            send_sum(step, 0, sums)
            ahead = apply(step + 2, image, step)
            norm, product = totals(wait_sum(step, 2))
        else:
            send_sum(step, 0, sums)
            send_sum(step, 1, wait_sum(step, 0))
            send_sum(step, 2, wait_sum(step, 1))
            norm, product = totals(wait_sum(step, 2))
        if step == 0:
            alpha = norm / product
            along_image = ahead
        else:
            ratio = norm / norm_before
            alpha = norm / (product - ratio * norm / alpha)
            direction = residual + ratio * direction
            if step + 1 < ITERS:
                along = image + ratio * along
                along_image = ahead + ratio * along_image
        answer = alpha * direction if answer is None else answer + alpha * direction
        norm_before = norm
        if step + 1 < ITERS:
            residual = residual - alpha * along
            image = image - alpha * along_image
    out[...] = answer
    for copy in sent:
        copy.wait_send()
    drain(ghosts[8], ghosts[9].at[0])
    drain(ghosts[19], ghosts[20].at[0])
    drain(slabs, ssend.at[0])
    if len(slots) > 1:
        at = pl.ds(1, len(slots) - 1)
        drain(nbuf.at[at], nsend.at[0])
        drain(fbuf.at[:, at], nsend.at[1])
    if direct and everyone:
        drain(dbuf.at[:, pl.ds(1, len(everyone))], dsend.at[0])


def ghost_scratch(sizes, beside, names, low, high):
    size_x, size_y, size_z = sizes
    fields, kinds = len(names), len(names) * (low + high)
    shapes = [
        (fields, low, size_y, size_z), (fields, high, size_y, size_z),
        (kinds, size_x, size_z), (kinds * low, size_z), (kinds * high, size_z),
        (beside, kinds, size_x, size_z), (beside, kinds * low, size_z), (beside, kinds * high, size_z),
        (fields * (low + high) * size_y + beside * kinds * (size_x + low + high), size_z),
    ]
    return [pltpu.VMEM(shape, jnp.float32) for shape in shapes] + [pltpu.SemaphoreType.DMA((1,))] * 2


def body(mesh_counts, density, base_velocity, cells, offsets, target, stiffness, counts):
    sizes = density.shape
    size_x, size_y, size_z = sizes
    cap = cells.shape[1]
    rows_y = size_y + 8
    groups = [axis_groups(count) for count in mesh_counts]
    number = len(groups[0]) * len(groups[1]) * len(groups[2])
    flat = len(groups[0]) * len(groups[1])
    tall_z, wide_xy = size_z + 16, round_up((size_x + 6) * rows_y, 128)
    longest = max(mesh_counts)
    turns = ITERS + 1
    devices = mesh_counts[0] * mesh_counts[1] * mesh_counts[2]
    most = devices if devices <= MOST_DIRECT else 1
    return pl.pallas_call(
        functools.partial(kernel, mesh_counts, sizes),
        out_shape=pltpu.VMEM((3, cap), jnp.float32),
        in_specs=[pl.BlockSpec(memory_space=pltpu.HBM)] * 7,
        out_specs=pl.BlockSpec(memory_space=pltpu.VMEM),
        scratch_shapes=[
            pltpu.VMEM((4, size_x, size_y, size_z), jnp.float32),
            pltpu.VMEM((size_x, size_y, size_z), jnp.float32),
            pltpu.VMEM((3, cap), jnp.int32),
            pltpu.VMEM((3, cap), jnp.float32),
            pltpu.VMEM((3, cap), jnp.float32),
            pltpu.VMEM((1, cap), jnp.float32),
            pltpu.SMEM((1,), jnp.int32),
            pltpu.VMEM((2, 8, rows_y * size_x), jnp.float32),
            pltpu.VMEM((number - flat, 2, 8, rows_y * size_x), jnp.float32),
            pltpu.VMEM((number, 8, cap), jnp.float32),
            pltpu.VMEM((ITERS, number, 3 * (cap // 128), 128), jnp.float32),
            pltpu.VMEM((ITERS, 3, longest, 2, 128), jnp.float32),
            pltpu.VMEM((ITERS, most, 2, 128), jnp.float32),
            pltpu.VMEM((wide_xy, number * cap), jnp.bfloat16),
            pltpu.VMEM((wide_xy, number * cap), jnp.bfloat16),
            pltpu.VMEM((tall_z, flat * cap), jnp.float32),
            pltpu.VMEM((8, max(1, len(groups[2]) - 1) * flat * cap), jnp.float32),
            pltpu.VMEM((6 * tall_z, flat * cap), jnp.bfloat16),
            pltpu.VMEM((4, tall_z, wide_xy), jnp.float32),
            pltpu.VMEM((3, tall_z, wide_xy), jnp.float32),
            pltpu.SemaphoreType.DMA((7,)),
            pltpu.SemaphoreType.DMA((2,)),
            pltpu.SemaphoreType.DMA((turns, STAGES)),
            pltpu.SemaphoreType.DMA((ITERS, 3, longest - 1) if most == 1 else (1, 1, 1)),
            pltpu.SemaphoreType.DMA((ITERS, 3, longest - 1) if most == 1 else (1, 1, 1)),
            pltpu.SemaphoreType.DMA((1,)),
            pltpu.SemaphoreType.DMA((ITERS,)),
            pltpu.SemaphoreType.DMA((1,)),
            pltpu.SemaphoreType.DMA((1,)),
        ] + [item for group in GHOSTS for item in ghost_scratch(sizes, len({1 % mesh_counts[1], (-1) % mesh_counts[1]}), *group)],
        compiler_params=pltpu.CompilerParams(
            collective_id=0, has_side_effects=True, vmem_limit_bytes=60 * 1024 * 1024
        ),
    )(density, base_velocity, cells, offsets, target, stiffness[None], counts)


def solution(mesh):
    return jax.shard_map(
        functools.partial(body, tuple(mesh.shape[name] for name in AXES)),
        mesh=mesh,
        in_specs=(
            P("gx", "gy", "gz"),
            P(None, "gx", "gy", "gz"),
            P(None, ("gx", "gy", "gz")),
            P(None, ("gx", "gy", "gz")),
            P(None, ("gx", "gy", "gz")),
            P(("gx", "gy", "gz")),
            P(("gx", "gy", "gz")),
        ),
        out_specs=P(None, ("gx", "gy", "gz")),
        check_vma=False,
    )
```
